32 devices in a mesh: orient: 8 (over z, y), dom: 4 (over x, core).
Axes of the slice: x: 2, y: 2, z: 4, core: 2. Of those that a mesh axis runs over, the one named last changes fastest.
Arguments:
- particles: bfloat16 [256, 8448], P(('dom', 'orient')), parts along dimension 0, may hold values from -12 to 12
- defocus: float32 [256], P(('dom', 'orient')), parts along dimension 0, may hold values from 10 to 60
- inv_noise: float32 [4224], replicated, may hold values from 0.5 to 2
- references: bfloat16 [13824, 8448], P(('dom', 'orient')), parts along dimension 0, may hold values from -0.25 to 0.25
- thresholds: int32 [256], P('dom'), parts along dimension 0, may hold values from 512 to 1023
- range_start: int32 [256], P('dom'), parts along dimension 0, may hold values from 0 to 3455
- range_len: int32 [256], P('dom'), parts along dimension 0, may hold values from 36 to 1727
Outputs:
- posterior: float32 [256, 3456], P('dom', 'orient'), parts along dimension 0
- cumulative: float32 [256, 3456], P('dom', 'orient'), parts along dimension 0
- log_evidence: float32 [256], P('dom'), parts along dimension 0
- kept_mass: float32 [256], P('dom'), parts along dimension 0
The draws below stay inside these ranges and needn't reach their ends.
There are 4 independent parts, one for each index of `dom`. The reference program is written for one: setup_inputs(seed, part) draws one part's arguments, and reference() takes and returns one part's arrays. A program takes and returns all parts, laid end to end along the dimension named above; an argument that names none is the same for every part. Nothing has to cross between parts.
All inputs are finite; a program needn't handle non-finite values.
Results may differ from the reference program's by a relative error of at most 0.0004.
The reference program's roundings to bfloat16 on the way (of `weighted`, `ctf_power` and `power`) count: a program that leaves them out, or rounds other values in their place, can miss the bound.
Values may be sent and summed in bfloat16 or wider, within the bound.
A program may use at most 64 MiB of HBM per device.

```python
import math
import jax
import jax.numpy as jnp
from jax import lax

COEF = 4224
FEAT = 8448
ROT = 36
ORIENTS = 3456
P_SIZE = 64


def ctf_rows(defocus, coef):
    index = jnp.arange(coef, dtype=jnp.int32)
    row_pos = (index // 128).astype(jnp.float32)
    col_pos = (index % 128 - 64).astype(jnp.float32)
    freq = math.pi * (row_pos * row_pos + col_pos * col_pos) / 16384.0
    return -jnp.sin(defocus[:, None] * freq[None, :] + 0.07)


def strong_rows(key):
    return jax.random.randint(jax.random.fold_in(key, 15), (8,), 0, ORIENTS)


def ref_row(key, row, strong):
    row_key = jax.random.fold_in(jax.random.fold_in(key, 11), row)
    spread = jnp.exp(jax.random.uniform(jax.random.fold_in(row_key, 1), (), jnp.float32, math.log(0.7), math.log(1.4)))
    base = jax.random.normal(jax.random.fold_in(row_key, 2), (FEAT,), jnp.float32)
    is_strong = jnp.any(strong == row)
    amplitude = jnp.where(is_strong, 0.12, 0.02)
    return jnp.clip(amplitude * spread * base, -0.25, 0.25)


def defocus_of(key):
    return jax.random.uniform(jax.random.fold_in(key, 12), (P_SIZE,), jnp.float32, 20.0, 50.0)


def draw_references(key, part):
    strong = strong_rows(key)
    rows_all = jnp.arange(ORIENTS, dtype=jnp.int32)
    return jax.vmap(lambda row: ref_row(key, row, strong))(rows_all).astype(jnp.bfloat16)


def draw_defocus(key, part):
    return defocus_of(key)


def draw_particles(key, part):
    images = jax.random.normal(jax.random.fold_in(key, 13), (P_SIZE, FEAT), jnp.float32)
    strong = strong_rows(key)
    chosen = jax.random.randint(jax.random.fold_in(key, 14), (4,), 0, P_SIZE)
    targets = jax.random.uniform(jax.random.fold_in(key, 16), (4,), jnp.float32, 110.0, 250.0)
    first_rows = jax.vmap(lambda row: ref_row(key, row, strong))(strong[:4])
    second_rows = jax.vmap(lambda row: ref_row(key, row, strong))(strong[4:])
    ctf = ctf_rows(defocus_of(key)[chosen], FEAT // 2)
    ctf_both = jnp.concatenate([ctf, ctf], axis=1)
    gain_first = targets / (0.0078 * FEAT)
    gain_second = (targets - 2.0) / (0.0078 * FEAT)
    aligned = 0.3 * images[chosen] + ctf_both * (gain_first[:, None] * first_rows + gain_second[:, None] * second_rows)
    images = images.at[chosen].set(aligned)
    return jnp.clip(images, -12.0, 12.0).astype(jnp.bfloat16)


def place_ends(result, stream_key, low, largest):
    shape = result.shape
    spot = [jax.random.randint(jax.random.fold_in(stream_key, axis), (), 0, shape[axis]) for axis in range(len(shape))]
    result = result.at[tuple(spot)].set(low)
    longest = shape.index(max(shape))
    spot[longest] = (spot[longest] + 1) % shape[longest]
    return result.at[tuple(spot)].set(largest)


def setup_inputs(seed: int = 0, part: int = 0) -> dict:
    key_of = jax.random.split(jax.random.key(seed), 8)
    part_keys = jax.random.split(jax.random.fold_in(key_of[7], part), 8)
    particles = draw_particles(jax.random.fold_in(jax.random.fold_in(key_of[7], part), 71), part)
    defocus = draw_defocus(jax.random.fold_in(jax.random.fold_in(key_of[7], part), 71), part)
    inv_noise = jnp.clip(jnp.exp(jax.random.uniform(key_of[2], (COEF,), jnp.float32, math.log(0.5), math.log(2.0))), 0.5, 2.0)
    references = draw_references(jax.random.fold_in(jax.random.fold_in(key_of[7], part), 71), part)
    thresholds = place_ends(jax.random.randint(part_keys[4], (P_SIZE,), 512, 1024), jax.random.fold_in(part_keys[4], 1), 512, 1023).astype(jnp.int32)
    range_start = place_ends(jax.random.randint(part_keys[5], (P_SIZE,), 0, ORIENTS), jax.random.fold_in(part_keys[5], 1), 0, ORIENTS - 1).astype(jnp.int32)
    range_len = place_ends(jax.random.randint(part_keys[6], (P_SIZE,), ROT, ORIENTS // 2), jax.random.fold_in(part_keys[6], 1), ROT, (ORIENTS // 2) - 1).astype(jnp.int32)
    return dict(particles=particles, defocus=defocus, inv_noise=inv_noise, references=references, thresholds=thresholds, range_start=range_start, range_len=range_len)


def ctf_table(defocus, coef):
    index = jnp.arange(coef, dtype=jnp.int32)
    row_pos = (index // 128).astype(jnp.float32)
    col_pos = (index % 128 - 64).astype(jnp.float32)
    freq = math.pi * (row_pos * row_pos + col_pos * col_pos) / 16384.0
    return -jnp.sin(defocus[:, None] * freq[None, :] + 0.07)


def reference(particles, defocus, inv_noise, references, thresholds, range_start, range_len):
    coef = inv_noise.shape[0]
    ctf = ctf_table(defocus, coef)
    ctf_both = jnp.concatenate([ctf, ctf], axis=1)
    noise_both = jnp.concatenate([inv_noise, inv_noise])
    weighted = (particles.astype(jnp.float32) * ctf_both * noise_both[None, :]).astype(jnp.bfloat16)
    ctf_power = (ctf * ctf * inv_noise[None, :]).astype(jnp.bfloat16)
    real_part = references[:, :coef].astype(jnp.float32)
    imag_part = references[:, coef:].astype(jnp.float32)
    power = (real_part * real_part + imag_part * imag_part).astype(jnp.bfloat16)
    dims = (((1,), (1,)), ((), ()))
    scores = lax.dot_general(weighted, references, dims, preferred_element_type=jnp.float32)
    scores = scores - 0.5 * lax.dot_general(ctf_power, power, dims, preferred_element_type=jnp.float32)
    top_score = jnp.max(scores, axis=1)
    expon = jnp.exp(scores - top_score[:, None])
    total = jnp.sum(expon, axis=1)
    posterior = expon / total[:, None]
    cumulative = jnp.cumsum(posterior, axis=1)
    before = cumulative - posterior
    fraction = thresholds.astype(jnp.float32) / 1024.0
    kept = jnp.minimum(jnp.maximum(fraction[:, None] - before, 0.0), posterior)
    orient_ids = jnp.arange(ORIENTS, dtype=jnp.int32)
    inside = ((orient_ids[None, :] - range_start[:, None]) % ORIENTS) < range_len[:, None]
    kept_mass = jnp.sum(jnp.where(inside, kept, 0.0), axis=1)
    log_evidence = top_score + jnp.log(total)
    return posterior, cumulative, log_evidence, kept_mass
```

```python
import functools
import math

import jax
import jax.numpy as jnp
from jax import lax
from jax.experimental import pallas as pl
from jax.experimental.pallas import tpu as pltpu
from jax.sharding import PartitionSpec as P

MESH = pl.DeviceIdType.MESH
DIMS = (((1,), (1,)), ((), ()))
PIECES = 3
SPANS = ((0, 4), (4, 6))
ROWS = 16


def sin_of(x):
    k = jnp.floor(x * (1.0 / math.pi) + 0.5)
    r = x - k * 3.140625
    r = r - k * 9.67502593994140625e-4
    r = r - k * 1.509957990978376432e-7
    s = r * r
    p = jnp.float32(-2.3889859e-8)
    p = p * s + 2.7525562e-6
    p = p * s - 1.9840874e-4
    p = p * s + 8.3333310e-3
    p = p * s - 1.6666667e-1
    y = r + r * s * p
    half = k * 0.5
    return jnp.where(half == jnp.floor(half), y, -y)


def loop(count, body):
    if count <= 4:
        for i in range(count):
            body(i)
    else:
        def step(i, carry):
            body(i)
            return carry
        lax.fori_loop(0, count, step, 0)


def kernel(
    n, particles, defocus, noise_hbm, references, starts_hbm, lens_hbm,
    expon, prefix, sgath,
    gath, dgath, refs, ctf, ctf_power, power, weighted, acc, mine, noise, starts, lens,
    own_sem, ref_sem, up_send, down_send, side_send, recv, dup_send, ddown_send, dside_send, d_recv, s_send, s_recv,
):
    wide = 2
    deep = n // wide
    per = particles.shape[0]
    feat = particles.shape[1]
    coef = feat // 2
    size = coef // PIECES
    ori = references.shape[0]
    total_ori = n * ori
    parts = n * per
    group = wide * per
    me = lax.axis_index("orient")
    row = lax.div(me, wide)
    col = lax.rem(me, wide)
    partner = row * wide + (1 - col)
    has_up = row + 1 < deep
    has_down = row > 0

    def cut(c):
        return pl.ds(c * size, size)

    def span(c):
        return pl.ds(SPANS[c][0] * size, (SPANS[c][1] - SPANS[c][0]) * size)

    def peer(t):
        return lax.rem(me + t, n)

    def near(act):
        act(partner)

        @pl.when(has_up)
        def _():
            act(me + wide)

        @pl.when(has_down)
        def _():
            act(me - wide)

    barrier = pltpu.get_barrier_semaphore()

    def greet(target):
        pl.semaphore_signal(barrier, inc=1, device_id={"orient": target}, device_id_type=MESH)

    near(greet)
    order = list(range(len(SPANS)))
    paired = -1
    pieces = [c for k in range(PIECES) for c in (k, k + PIECES)]
    own = pltpu.make_async_copy(particles, gath.at[me], own_sem.at[0])
    own.start()
    own_d = pltpu.make_async_copy(defocus, dgath.at[me], own_sem.at[1])
    own_d.start()
    loads = {}
    for c in pieces:
        loads[c] = pltpu.make_async_copy(references.at[:, cut(c)], refs.at[:, cut(c)], ref_sem.at[c])
        loads[c].start()
    small = [
        pltpu.make_async_copy(noise_hbm, noise, own_sem.at[2]),
        pltpu.make_async_copy(starts_hbm, starts, own_sem.at[3]),
        pltpu.make_async_copy(lens_hbm, lens, own_sem.at[4]),
    ]
    for copy in small:
        copy.start()
    own.wait()
    own_d.wait()
    pl.semaphore_wait(barrier, 1 + has_up.astype(jnp.int32) + has_down.astype(jnp.int32))

    def remote(block, send_sem, recv_sem, target):
        return pltpu.make_async_remote_copy(
            src_ref=block, dst_ref=block, send_sem=send_sem, recv_sem=recv_sem,
            device_id={"orient": target}, device_id_type=MESH)

    def up(c, source):
        if c is None:
            return remote(dgath.at[source], dup_send.at[source], d_recv.at[source], me + wide)
        return remote(gath.at[source, :, span(c)], up_send.at[c, source], recv.at[c, source], me + wide)

    def down(c, source):
        if c is None:
            return remote(dgath.at[source], ddown_send.at[source], d_recv.at[source], me - wide)
        return remote(gath.at[source, :, span(c)], down_send.at[c, source], recv.at[c, source], me - wide)

    def side(c, source):
        if c is None:
            return remote(dgath.at[source], dside_send.at[source], d_recv.at[source], partner)
        return remote(gath.at[source, :, span(c)], side_send.at[c, source], recv.at[c, source], partner)

    def s_copy(source, target):
        return pltpu.make_async_remote_copy(
            src_ref=mine, dst_ref=sgath.at[source],
            send_sem=s_send.at[target], recv_sem=s_recv.at[source],
            device_id={"orient": target}, device_id_type=MESH)

    def both(c, source):
        @pl.when(has_up)
        def _():
            up(c, source).start()

        @pl.when(has_down)
        def _():
            down(c, source).start()

    side(None, me).start()
    both(None, me)
    for c in order:
        side(c, me).start()
    for c in order:
        both(c, me)

    def handle(c, t):
        @pl.when(row >= t)
        def _():
            for column in (col, 1 - col) if c == paired else (col,):
                source = (row - t) * wide + column
                side(c, source).wait_recv()

                @pl.when(has_up)
                def _():
                    up(c, source).start()

                if c != paired:
                    side(c, source).start()

        @pl.when(row + t < deep)
        def _():
            for column in (col, 1 - col) if c == paired else (col,):
                source = (row + t) * wide + column
                side(c, source).wait_recv()

                @pl.when(has_down)
                def _():
                    down(c, source).start()

                if c != paired:
                    side(c, source).start()

    def arrived(c):
        if c != paired:
            for r in range(deep):
                side(c, r * wide + 1 - col).wait_recv()

    eye8 = lax.broadcasted_iota(jnp.int32, (per, per), 0) == lax.broadcasted_iota(jnp.int32, (per, per), 1)

    def ctf_row(r, wait=True):
        if wait:
            side(None, r * wide + 1 - col).wait_recv()
        columns = []
        for j in range(wide):
            columns.append(jnp.sum(jnp.where(eye8, dgath[r * wide + j], 0.0), axis=1, keepdims=True))
        d = jnp.concatenate(columns, axis=0)
        rows = pl.ds(pl.multiple_of(r * group, group), group)

        def body(k):
            index = k * size + lax.broadcasted_iota(jnp.int32, (1, size), 1)
            row_pos = lax.shift_right_logical(index, 7).astype(jnp.float32)
            col_pos = ((index & 127) - 64).astype(jnp.float32)
            freq = math.pi * (row_pos * row_pos + col_pos * col_pos) / 16384.0
            value = -sin_of(d * freq + 0.07)
            ctf[rows, cut(k)] = value
            ctf_power[rows, cut(k)] = (value * value * noise[cut(k)].reshape(1, size)).astype(jnp.bfloat16)

        for k in range(PIECES):
            body(k)

    def ctf_rows(t):
        @pl.when(row >= t)
        def _():
            ctf_row(row - t)

        @pl.when(row + t < deep)
        def _():
            ctf_row(row + t)

    def power_piece(k):
        loads[k].wait()
        loads[k + PIECES].wait()

        def body(i):
            rows = pl.ds(pl.multiple_of(i * ROWS, ROWS), ROWS)
            re = refs[rows, cut(k)].astype(jnp.float32)
            im = refs[rows, cut(k + PIECES)].astype(jnp.float32)
            power[rows, cut(k)] = (re * re + im * im).astype(jnp.bfloat16)

        loop(ori // ROWS, body)

    def energy_piece(k):
        term = -0.5 * lax.dot_general(
            ctf_power[:, cut(k)], power[:, cut(k)], DIMS, preferred_element_type=jnp.float32)
        if k == 0:
            acc[...] = term
        else:
            acc[...] += term

    def cross_piece(c):
        k = c % PIECES

        def body(i):
            rows = pl.ds(pl.multiple_of(i * group, group), group)
            block = gath[pl.ds(i * wide, wide), :, cut(c)].astype(jnp.float32).reshape(group, size)
            weighted[rows, :] = (block * ctf[rows, cut(k)] * noise[cut(k)].reshape(1, size)).astype(jnp.bfloat16)

        loop(deep, body)
        acc[...] += lax.dot_general(weighted[...], refs[:, cut(c)], DIMS, preferred_element_type=jnp.float32)

    short = deep == 4
    power_piece(0)
    power_piece(1)
    for copy in small:
        copy.wait()
    if short:
        tasks = {
            (1, 0): [lambda: ctf_row(row)],
            (1, 1): [lambda: power_piece(2), lambda: ctf_rows(1)],
            (2, 1): [lambda: ctf_rows(2)],
            (3, 0): [lambda: ctf_rows(3), lambda: energy_piece(0)],
            (3, 1): [lambda: energy_piece(1), lambda: energy_piece(2)],
        }
    else:
        tasks = {(1, 0): [lambda: power_piece(2)]}
    for t in range(1, deep):
        handle(None, t)
        for i, c in enumerate(order):
            handle(c, t)
            for task in tasks.get((t, i), ()):
                task()
    if not short:
        for r in range(deep):
            side(None, r * wide + 1 - col).wait_recv()
        loop(deep, lambda r: ctf_row(r, wait=False))
        for k in range(PIECES):
            energy_piece(k)
    for c in order:
        arrived(c)
        for piece in range(*SPANS[c]):
            cross_piece(piece)

    scores = acc[...]
    top = jnp.max(scores, axis=1, keepdims=True)
    e = jnp.exp(scores - top)
    expon[:, :ori] = e
    eye = lax.broadcasted_iota(jnp.int32, (parts, parts), 0) == lax.broadcasted_iota(jnp.int32, (parts, parts), 1)

    def to_col(x):
        return jnp.sum(jnp.where(eye, x, 0), axis=1, keepdims=True)

    def to_row(x):
        return jnp.sum(jnp.where(eye, x, 0.0), axis=0, keepdims=True)

    start = to_col(starts[...])
    length = to_col(lens[...])
    ids = me * ori + lax.broadcasted_iota(jnp.int32, (parts, ori), 1)
    rel = ids - start
    inside = jnp.where(rel < 0, rel + total_ori, rel) < length
    first = me * ori - start
    first_inside = jnp.where(first < 0, first + total_ori, first) < length
    in_range = jnp.sum(jnp.where(inside, e, 0.0), axis=1, keepdims=True)
    ahead = jnp.sum(jnp.where(rel < 0, e, 0.0), axis=1, keepdims=True)
    ahead = jnp.where(first_inside, 0.0, ahead)
    for i, value in enumerate((top, jnp.sum(e, axis=1, keepdims=True), in_range, ahead)):
        line = to_row(value)
        mine[i : i + 1, :] = line
        sgath[me, i : i + 1, :] = line
    for t in range(1, n):
        s_copy(me, peer(t)).start()

    lanes = 128
    blocks = expon.shape[1] // lanes
    if ori < expon.shape[1]:
        expon[:, ori:] = jnp.zeros((parts, expon.shape[1] - ori), jnp.float32)
    upper = (
        lax.broadcasted_iota(jnp.int32, (lanes, lanes), 0) <= lax.broadcasted_iota(jnp.int32, (lanes, lanes), 1)
    ).astype(jnp.bfloat16)
    carry = jnp.zeros((parts, 1), jnp.float32)
    for b in range(blocks):
        x = expon[:, b * lanes : (b + 1) * lanes]
        high = x.astype(jnp.bfloat16)
        rest = x - high.astype(jnp.float32)
        mid = rest.astype(jnp.bfloat16)
        low = (rest - mid.astype(jnp.float32)).astype(jnp.bfloat16)
        run = carry
        for piece in (low, mid, high):
            run = run + jnp.dot(piece, upper, preferred_element_type=jnp.float32)
        prefix[:, b * lanes : (b + 1) * lanes] = run
        carry = run[:, lanes - 1 : lanes]

    def drain(c, source, along, across):
        if along:
            @pl.when(has_up & (lax.div(source, wide) <= row))
            def _():
                up(c, source).wait_send()

            @pl.when(has_down & (lax.div(source, wide) >= row))
            def _():
                down(c, source).wait_send()

        if across:
            side(c, source).wait_send()

    for c in [None] + order:
        for r in range(deep):
            drain(c, r * wide + col, True, c != paired)
            if c == paired:
                drain(c, r * wide + 1 - col, True, False)
    for t in range(1, n):
        s_copy(me, peer(t)).wait_send()
    for t in range(1, n):
        s_copy(peer(t), me).wait_recv()


def finish(n, expon, prefix, sgath, thresholds, posterior, cumulative, evidence, kept_mass):
    parts, ori = posterior.shape
    me = lax.axis_index("orient")
    eye = lax.broadcasted_iota(jnp.int32, (parts, parts), 0) == lax.broadcasted_iota(jnp.int32, (parts, parts), 1)

    def to_col(x):
        return jnp.sum(jnp.where(eye, x, 0), axis=1, keepdims=True)

    stats = [sgath[s] for s in range(n)]
    best = stats[0][0:1]
    for s in stats[1:]:
        best = jnp.maximum(best, s[0:1])
    scale = [jnp.exp(s[0:1] - best) for s in stats]
    base = jnp.zeros_like(best)
    my_base = base
    bases = []
    for s in range(n):
        my_base = jnp.where(me == s, base, my_base)
        bases.append(base)
        base = base + scale[s] * stats[s][1:2]
    total = base
    limit = thresholds[...].astype(jnp.float32) / 1024.0 * total
    kept = jnp.zeros_like(best)
    for s in range(n):
        left = limit - bases[s] - scale[s] * stats[s][3:4]
        kept = kept + jnp.minimum(jnp.maximum(left, 0.0), scale[s] * stats[s][2:3])
    kept_mass[...] = kept / total
    evidence[...] = best + jnp.log(total)
    my_scale = to_col(jnp.exp(sgath[me, 0:1, :] - best) / total)
    my_base = to_col(my_base / total)
    posterior[...] = expon[:, :ori] * my_scale
    cumulative[...] = my_base + prefix[:, :ori] * my_scale


def on_device(n, particles, defocus, inv_noise, references, thresholds, range_start, range_len):
    per, feat = particles.shape
    coef = feat // 2
    ori = references.shape[0]
    parts = n * per
    padded = -(-ori // 128) * 128
    chunks = 2 * PIECES
    f32, bf16 = jnp.float32, jnp.bfloat16
    vmem = pl.BlockSpec(memory_space=pltpu.VMEM)
    hbm = pl.BlockSpec(memory_space=pl.ANY)
    dma = pltpu.SemaphoreType.DMA
    expon, prefix, stats = pl.pallas_call(
        functools.partial(kernel, n),
        out_shape=(
            pltpu.VMEM((parts, padded), f32),
            pltpu.VMEM((parts, padded), f32),
            pltpu.VMEM((n, 4, parts), f32),
        ),
        in_specs=[hbm] * 6,
        out_specs=[vmem] * 3,
        scratch_shapes=[
            pltpu.VMEM((n, per, feat), bf16),
            pltpu.VMEM((n, 1, per), f32),
            pltpu.VMEM((ori, feat), bf16),
            pltpu.VMEM((parts, coef), f32),
            pltpu.VMEM((parts, coef), bf16),
            pltpu.VMEM((ori, coef), bf16),
            pltpu.VMEM((parts, coef // PIECES), bf16),
            pltpu.VMEM((parts, ori), f32),
            pltpu.VMEM((4, parts), f32),
            pltpu.VMEM((coef,), f32),
            pltpu.VMEM((1, parts), jnp.int32),
            pltpu.VMEM((1, parts), jnp.int32),
            dma((5,)),
            dma((chunks,)),
            dma((len(SPANS), n)),
            dma((len(SPANS), n)),
            dma((len(SPANS), n)),
            dma((len(SPANS), n)),
            dma((n,)),
            dma((n,)),
            dma((n,)),
            dma((n,)),
            dma((n,)),
            dma((n,)),
        ],
        compiler_params=pltpu.CompilerParams(
            collective_id=0, has_side_effects=True, vmem_limit_bytes=48 * 1024 * 1024
        ),
    )(*(
        pltpu.with_memory_space_constraint(x, pltpu.HBM) for x in (
            particles, defocus.reshape(1, per), inv_noise, references,
            range_start.reshape(1, parts), range_len.reshape(1, parts))
    ))
    outs = pl.pallas_call(
        functools.partial(finish, n),
        out_shape=(
            jax.ShapeDtypeStruct((parts, ori), f32),
            jax.ShapeDtypeStruct((parts, ori), f32),
            jax.ShapeDtypeStruct((1, parts), f32),
            jax.ShapeDtypeStruct((1, parts), f32),
        ),
        in_specs=[vmem] * 4,
        out_specs=[vmem] * 4,
        compiler_params=pltpu.CompilerParams(vmem_limit_bytes=8 * 1024 * 1024),
    )(expon, prefix, stats, thresholds.reshape(1, parts))
    return outs[0], outs[1], outs[2].reshape(parts), outs[3].reshape(parts)


def solution(mesh):
    return jax.shard_map(
        functools.partial(on_device, mesh.shape["orient"]),
        mesh=mesh,
        in_specs=(
            P(("dom", "orient"), None),
            P(("dom", "orient")),
            P(),
            P(("dom", "orient"), None),
            P("dom"),
            P("dom"),
            P("dom"),
        ),
        out_specs=(P("dom", "orient"), P("dom", "orient"), P("dom"), P("dom")),
        check_vma=False,
    )
```

```python
import functools
import math

import jax
import jax.numpy as jnp
from jax import lax
from jax.experimental import pallas as pl
from jax.experimental.pallas import tpu as pltpu
from jax.sharding import PartitionSpec as P

MESH = pl.DeviceIdType.MESH
DIMS = (((1,), (1,)), ((), ()))
PIECES = 3
SPANS = ((0, 4), (4, 6))
ORDER = tuple(c for k in range(PIECES) for c in (k, k + PIECES))
ROWS = 16


def sin_of(x):
    k = jnp.floor(x * (1.0 / math.pi) + 0.5)
    r = x - k * 3.140625
    r = r - k * 9.67502593994140625e-4
    r = r - k * 1.509957990978376432e-7
    s = r * r
    p = jnp.float32(-2.3889859e-8)
    p = p * s + 2.7525562e-6
    p = p * s - 1.9840874e-4
    p = p * s + 8.3333310e-3
    p = p * s - 1.6666667e-1
    y = r + r * s * p
    half = k * 0.5
    return jnp.where(half == jnp.floor(half), y, -y)


def loop(count, body):
    if count <= 4:
        for i in range(count):
            body(i)
    else:
        def step(i, carry):
            body(i)
            return carry
        lax.fori_loop(0, count, step, 0)


def kernel(
    n, particles, defocus, noise_hbm, references, starts_hbm, lens_hbm,
    expon, prefix, sgath,
    gath, dgath, refs, ctf, ctf_power, power, weighted, acc, mine, noise, starts, lens,
    own_sem, piece_sem, ref_sem, up_send, down_send, side_send, recv, side_recv,
    dup_send, ddown_send, beside_send, beside_recv, pair_recv, far_send, far_recv, s_send, s_recv,
):
    wide = 2
    deep = n // wide
    per = particles.shape[0]
    feat = particles.shape[1]
    coef = feat // 2
    size = coef // PIECES
    ori = references.shape[0]
    total_ori = n * ori
    parts = n * per
    group = wide * per
    me = lax.axis_index("orient")
    row = lax.div(me, wide)
    col = lax.rem(me, wide)
    partner = row * wide + (1 - col)
    has_up = row + 1 < deep
    has_down = row > 0

    def cut(c):
        return pl.ds(c * size, size)

    short = deep == 4
    spans = [(c, c + 1) for c in ORDER] if short else SPANS
    lowest, highest = row == 0, row == deep - 1

    def span(c):
        return pl.ds(spans[c][0] * size, (spans[c][1] - spans[c][0]) * size)

    def peer(t):
        return lax.rem(me + t, n)

    def near(act):
        act(partner)

        @pl.when(has_up)
        def _():
            act(me + wide)

        @pl.when(has_down)
        def _():
            act(me - wide)

    barrier = pltpu.get_barrier_semaphore()

    def greet(target):
        pl.semaphore_signal(barrier, inc=1, device_id={"orient": target}, device_id_type=MESH)

    near(greet)
    if short:
        @pl.when(lowest)
        def _():
            for column in range(wide):
                greet((deep - 1) * wide + column)

    order = list(range(len(spans)))
    own = [
        pltpu.make_async_copy(particles.at[:, span(c)], gath.at[me, :, span(c)], piece_sem.at[c])
        for c in order
    ]
    own_d = pltpu.make_async_copy(defocus, dgath.at[me], own_sem.at[1])
    own_d.start()
    for copy in own:
        copy.start()
    for c in ORDER:
        pltpu.make_async_copy(references.at[:, cut(c)], refs.at[:, cut(c)], ref_sem.at[c % PIECES]).start()
    small = [
        pltpu.make_async_copy(noise_hbm, noise, own_sem.at[2]),
        pltpu.make_async_copy(starts_hbm, starts, own_sem.at[3]),
        pltpu.make_async_copy(lens_hbm, lens, own_sem.at[4]),
    ]
    for copy in small:
        copy.start()
    own_d.wait()
    greeted = 1 + has_up.astype(jnp.int32) + has_down.astype(jnp.int32)
    if short:
        greeted = greeted + wide * highest.astype(jnp.int32)
    pl.semaphore_wait(barrier, greeted)

    def remote(block, send_sem, recv_sem, target):
        return pltpu.make_async_remote_copy(
            src_ref=block, dst_ref=block, send_sem=send_sem, recv_sem=recv_sem,
            device_id={"orient": target}, device_id_type=MESH)

    def block(c, source):
        return gath.at[source, :, span(c)]

    def up(c, source):
        return remote(block(c, source), up_send, recv.at[c, lax.div(source, wide)], me + wide)

    def down(c, source):
        return remote(block(c, source), down_send, recv.at[c, lax.div(source, wide)], me - wide)

    def side(c, source):
        return remote(block(c, source), side_send, side_recv.at[c], partner)

    def beside(source):
        return remote(dgath.at[source], beside_send, beside_recv, partner)

    def pair(r):
        return dgath.at[pl.ds(r * wide, wide)]

    def pair_up(r):
        return remote(pair(r), dup_send, pair_recv.at[r], me + wide)

    def pair_down(r):
        return remote(pair(r), ddown_send, pair_recv.at[r], me - wide)

    def s_copy(source, target):
        return pltpu.make_async_remote_copy(
            src_ref=mine, dst_ref=sgath.at[source], send_sem=s_send, recv_sem=s_recv,
            device_id={"orient": target}, device_id_type=MESH)

    others = sgath.at[pl.ds(0, n - 1)]

    def both(c, source):
        @pl.when(has_up)
        def _():
            up(c, source).start()

        @pl.when(has_down)
        def _():
            down(c, source).start()

    def far(column):
        return remote(dgath.at[me], far_send, far_recv.at[col], column)

    far_both = remote(pair(deep - 1), far_send, far_recv.at[0], partner)

    if short:
        @pl.when(highest)
        def _():
            for column in range(wide):
                far(column).start()

    beside(me).start()
    for c in order:
        own[c].wait()
        side(c, me).start()
        both(c, me)

    def relay_pairs(t):
        if t == 0:
            beside(partner).wait_recv()

            @pl.when(has_up)
            def _():
                pair_up(row).start()

            @pl.when(has_down)
            def _():
                pair_down(row).start()

            return

        @pl.when(row >= t)
        def _():
            pair_up(row - t).wait_recv()

            @pl.when(has_up)
            def _():
                pair_up(row - t).start()

        direct = short and t == deep - 1

        @pl.when(row + t < deep)
        def _():
            if direct:
                for column in range(wide):
                    source = (deep - 1) * wide + column
                    remote(dgath.at[source], far_send, far_recv.at[column], partner).wait_recv()
            else:
                pair_down(row + t).wait_recv()

                @pl.when(has_down & (row > 1 if short and t == deep - 2 else True))
                def _():
                    pair_down(row + t).start()

    def handle(c, t):
        @pl.when(row >= t)
        def _():
            source = (row - t) * wide + col
            up(c, source).wait_recv()

            @pl.when(has_up)
            def _():
                up(c, source).start()

            side(c, source).start()

        @pl.when(row + t < deep)
        def _():
            source = (row + t) * wide + col
            down(c, source).wait_recv()

            @pl.when(has_down)
            def _():
                down(c, source).start()

            side(c, source).start()

    def arrived(c):
        blocks = gath.at[pl.ds(0, deep), :, span(c)]
        remote(blocks, side_send, side_recv.at[c], partner).wait_recv()

    eye8 = lax.broadcasted_iota(jnp.int32, (per, per), 0) == lax.broadcasted_iota(jnp.int32, (per, per), 1)

    def ctf_row(r):
        columns = []
        for j in range(wide):
            columns.append(jnp.sum(jnp.where(eye8, dgath[r * wide + j], 0.0), axis=1, keepdims=True))
        d = jnp.concatenate(columns, axis=0)
        rows = pl.ds(pl.multiple_of(r * group, group), group)

        def body(k):
            index = k * size + lax.broadcasted_iota(jnp.int32, (1, size), 1)
            row_pos = lax.shift_right_logical(index, 7).astype(jnp.float32)
            col_pos = ((index & 127) - 64).astype(jnp.float32)
            freq = math.pi * (row_pos * row_pos + col_pos * col_pos) / 16384.0
            value = -sin_of(d * freq + 0.07)
            ctf[rows, cut(k)] = value
            ctf_power[rows, cut(k)] = (value * value * noise[cut(k)].reshape(1, size)).astype(jnp.bfloat16)

        for k in range(PIECES):
            body(k)

    def ctf_rows(t):
        @pl.when(row >= t)
        def _():
            ctf_row(row - t)

        @pl.when(row + t < deep)
        def _():
            ctf_row(row + t)

    def power_piece(k):
        both_parts = pl.ds(0, 2 * size)
        pltpu.make_async_copy(references.at[:, both_parts], refs.at[:, both_parts], ref_sem.at[k]).wait()

        def body(i):
            rows = pl.ds(pl.multiple_of(i * ROWS, ROWS), ROWS)
            re = refs[rows, cut(k)].astype(jnp.float32)
            im = refs[rows, cut(k + PIECES)].astype(jnp.float32)
            power[rows, cut(k)] = (re * re + im * im).astype(jnp.bfloat16)

        loop(ori // ROWS, body)

    def energy_piece(k):
        term = -0.5 * lax.dot_general(
            ctf_power[:, cut(k)], power[:, cut(k)], DIMS, preferred_element_type=jnp.float32)
        if k == 0:
            acc[...] = term
        else:
            acc[...] += term

    def cross_piece(c):
        k = c % PIECES

        def body(i):
            rows = pl.ds(pl.multiple_of(i * group, group), group)
            block = gath[pl.ds(i * wide, wide), :, cut(c)].astype(jnp.float32).reshape(group, size)
            weighted[rows, :] = (block * ctf[rows, cut(k)] * noise[cut(k)].reshape(1, size)).astype(jnp.bfloat16)

        loop(deep, body)
        acc[...] += lax.dot_general(weighted[...], refs[:, cut(c)], DIMS, preferred_element_type=jnp.float32)

    power_piece(0)
    power_piece(1)
    for copy in small:
        copy.wait()
    if short:
        tasks = {
            (1, 0): [lambda: power_piece(2)],
            (1, 1): [lambda: ctf_row(row)],
            (1, 5): [lambda: relay_pairs(1)],
            (2, 0): [lambda: ctf_rows(1)],
            (2, 3): [lambda: relay_pairs(2)],
            (2, 4): [lambda: ctf_rows(2)],
            (3, 1): [lambda: relay_pairs(3), lambda: ctf_rows(3)],
            (3, 2): [lambda: energy_piece(0)],
            (3, 3): [lambda: energy_piece(1)],
            (3, 4): [lambda: energy_piece(2)],
        }
    else:
        tasks = {(1, 0): [lambda: power_piece(2)]}
    relay_pairs(0)
    for t in range(1, deep):
        if not short:
            relay_pairs(t)
        for c in order:
            handle(c, t)
            for task in tasks.get((t, c), ()):
                task()
    if not short:
        loop(deep, ctf_row)
        for k in range(PIECES):
            energy_piece(k)
    for c in order:
        arrived(c)
        for piece in range(*spans[c]):
            cross_piece(piece)

    scores = acc[...]
    top = jnp.max(scores, axis=1, keepdims=True)
    e = jnp.exp(scores - top)
    expon[:, :ori] = e
    eye = lax.broadcasted_iota(jnp.int32, (parts, parts), 0) == lax.broadcasted_iota(jnp.int32, (parts, parts), 1)

    def to_col(x):
        return jnp.sum(jnp.where(eye, x, 0), axis=1, keepdims=True)

    def to_row(x):
        return jnp.sum(jnp.where(eye, x, 0.0), axis=0, keepdims=True)

    start = to_col(starts[...])
    length = to_col(lens[...])
    ids = me * ori + lax.broadcasted_iota(jnp.int32, (parts, ori), 1)
    rel = ids - start
    inside = jnp.where(rel < 0, rel + total_ori, rel) < length
    first = me * ori - start
    first_inside = jnp.where(first < 0, first + total_ori, first) < length
    in_range = jnp.sum(jnp.where(inside, e, 0.0), axis=1, keepdims=True)
    ahead = jnp.sum(jnp.where(rel < 0, e, 0.0), axis=1, keepdims=True)
    ahead = jnp.where(first_inside, 0.0, ahead)
    for i, value in enumerate((top, jnp.sum(e, axis=1, keepdims=True), in_range, ahead)):
        line = to_row(value)
        mine[i : i + 1, :] = line
        sgath[me, i : i + 1, :] = line
    for t in range(1, n):
        s_copy(me, peer(t)).start()

    lanes = 128
    blocks = expon.shape[1] // lanes
    if ori < expon.shape[1]:
        expon[:, ori:] = jnp.zeros((parts, expon.shape[1] - ori), jnp.float32)
    upper = (
        lax.broadcasted_iota(jnp.int32, (lanes, lanes), 0) <= lax.broadcasted_iota(jnp.int32, (lanes, lanes), 1)
    ).astype(jnp.bfloat16)
    carry = jnp.zeros((parts, 1), jnp.float32)
    for b in range(blocks):
        x = expon[:, b * lanes : (b + 1) * lanes]
        high = x.astype(jnp.bfloat16)
        rest = x - high.astype(jnp.float32)
        mid = rest.astype(jnp.bfloat16)
        low = (rest - mid.astype(jnp.float32)).astype(jnp.bfloat16)
        run = carry
        for piece in (low, mid, high):
            run = run + jnp.dot(piece, upper, preferred_element_type=jnp.float32)
        prefix[:, b * lanes : (b + 1) * lanes] = run
        carry = run[:, lanes - 1 : lanes]

    def sent(blocks, pairs, send_sem, pair_sem):
        remote(gath.at[pl.ds(0, blocks)], send_sem, side_recv.at[0], partner).wait_send()
        remote(dgath.at[pl.ds(0, pairs * wide)], pair_sem, beside_recv, partner).wait_send()

    beside(me).wait_send()
    remote(gath.at[pl.ds(0, deep)], side_send, side_recv.at[0], partner).wait_send()
    for r in range(deep - 1):
        @pl.when(row == r)
        def _():
            sent(r + 1, r + 1, up_send, dup_send)

        @pl.when(row == deep - 1 - r)
        def _():
            skipped = short and r == deep - 2
            sent(r + 1, r if skipped else r + 1, down_send, ddown_send)

    if short:
        @pl.when(highest)
        def _():
            far_both.wait_send()

    remote(others, s_send, s_recv, partner).wait_send()
    remote(others, s_send, s_recv, partner).wait_recv()


def finish(n, expon, prefix, sgath, thresholds, posterior, cumulative, evidence, kept_mass):
    parts, ori = posterior.shape
    me = lax.axis_index("orient")
    eye = lax.broadcasted_iota(jnp.int32, (parts, parts), 0) == lax.broadcasted_iota(jnp.int32, (parts, parts), 1)

    def to_col(x):
        return jnp.sum(jnp.where(eye, x, 0), axis=1, keepdims=True)

    stats = [sgath[s] for s in range(n)]
    best = stats[0][0:1]
    for s in stats[1:]:
        best = jnp.maximum(best, s[0:1])
    scale = [jnp.exp(s[0:1] - best) for s in stats]
    base = jnp.zeros_like(best)
    my_base = base
    bases = []
    for s in range(n):
        my_base = jnp.where(me == s, base, my_base)
        bases.append(base)
        base = base + scale[s] * stats[s][1:2]
    total = base
    limit = thresholds[...].astype(jnp.float32) / 1024.0 * total
    kept = jnp.zeros_like(best)
    for s in range(n):
        left = limit - bases[s] - scale[s] * stats[s][3:4]
        kept = kept + jnp.minimum(jnp.maximum(left, 0.0), scale[s] * stats[s][2:3])
    kept_mass[...] = kept / total
    evidence[...] = best + jnp.log(total)
    my_scale = to_col(jnp.exp(sgath[me, 0:1, :] - best) / total)
    my_base = to_col(my_base / total)
    posterior[...] = expon[:, :ori] * my_scale
    cumulative[...] = my_base + prefix[:, :ori] * my_scale


def on_device(n, particles, defocus, inv_noise, references, thresholds, range_start, range_len):
    per, feat = particles.shape
    coef = feat // 2
    ori = references.shape[0]
    parts = n * per
    padded = -(-ori // 128) * 128
    chunks = 2 * PIECES
    f32, bf16 = jnp.float32, jnp.bfloat16
    vmem = pl.BlockSpec(memory_space=pltpu.VMEM)
    hbm = pl.BlockSpec(memory_space=pl.ANY)
    dma = pltpu.SemaphoreType.DMA
    expon, prefix, stats = pl.pallas_call(
        functools.partial(kernel, n),
        out_shape=(
            pltpu.VMEM((parts, padded), f32),
            pltpu.VMEM((parts, padded), f32),
            pltpu.VMEM((n, 4, parts), f32),
        ),
        in_specs=[hbm] * 6,
        out_specs=[vmem] * 3,
        scratch_shapes=[
            pltpu.VMEM((n, per, feat), bf16),
            pltpu.VMEM((n, 1, per), f32),
            pltpu.VMEM((ori, feat), bf16),
            pltpu.VMEM((parts, coef), f32),
            pltpu.VMEM((parts, coef), bf16),
            pltpu.VMEM((ori, coef), bf16),
            pltpu.VMEM((parts, coef // PIECES), bf16),
            pltpu.VMEM((parts, ori), f32),
            pltpu.VMEM((4, parts), f32),
            pltpu.VMEM((coef,), f32),
            pltpu.VMEM((1, parts), jnp.int32),
            pltpu.VMEM((1, parts), jnp.int32),
            dma((5,)),
            dma((chunks,)),
            dma((PIECES,)),
            dma, dma, dma,
            dma((chunks, n // 2)),
            dma((chunks,)),
            dma, dma, dma, dma,
            dma((n // 2,)),
            dma,
            dma((2,)),
            dma, dma,
        ],
        compiler_params=pltpu.CompilerParams(
            collective_id=0, has_side_effects=True, vmem_limit_bytes=48 * 1024 * 1024
        ),
    )(*(
        pltpu.with_memory_space_constraint(x, pltpu.HBM) for x in (
            particles, defocus.reshape(1, per), inv_noise, references,
            range_start.reshape(1, parts), range_len.reshape(1, parts))
    ))
    outs = pl.pallas_call(
        functools.partial(finish, n),
        out_shape=(
            jax.ShapeDtypeStruct((parts, ori), f32),
            jax.ShapeDtypeStruct((parts, ori), f32),
            jax.ShapeDtypeStruct((1, parts), f32),
            jax.ShapeDtypeStruct((1, parts), f32),
        ),
        in_specs=[vmem] * 4,
        out_specs=[vmem] * 4,
        compiler_params=pltpu.CompilerParams(vmem_limit_bytes=8 * 1024 * 1024),
    )(expon, prefix, stats, thresholds.reshape(1, parts))
    return outs[0], outs[1], outs[2].reshape(parts), outs[3].reshape(parts)


def solution(mesh):
    return jax.shard_map(
        functools.partial(on_device, mesh.shape["orient"]),
        mesh=mesh,
        in_specs=(
            P(("dom", "orient"), None),
            P(("dom", "orient")),
            P(),
            P(("dom", "orient"), None),
            P("dom"),
            P("dom"),
            P("dom"),
        ),
        out_specs=(P("dom", "orient"), P("dom", "orient"), P("dom"), P("dom")),
        check_vma=False,
    )
```

```python
import functools
import math

import jax
import jax.numpy as jnp
from jax import lax
from jax.experimental import pallas as pl
from jax.experimental.pallas import tpu as pltpu
from jax.sharding import PartitionSpec as P

MESH = pl.DeviceIdType.MESH
DIMS = (((1,), (1,)), ((), ()))
PIECES = 3
SPANS = ((0, 4), (4, 6))
EARLY = 1
STEPS = ((0,), (1, 2), (3, 4, 5))
ORDER = tuple(c for k in range(PIECES) for c in (k, k + PIECES))
ROWS = 16


def sin_of(x):
    k = jnp.floor(x * (1.0 / math.pi) + 0.5)
    r = x - k * 3.140625
    r = r - k * 9.67502593994140625e-4
    r = r - k * 1.509957990978376432e-7
    s = r * r
    p = jnp.float32(-2.3889859e-8)
    p = p * s + 2.7525562e-6
    p = p * s - 1.9840874e-4
    p = p * s + 8.3333310e-3
    p = p * s - 1.6666667e-1
    y = r + r * s * p
    half = k * 0.5
    return jnp.where(half == jnp.floor(half), y, -y)


def loop(count, body):
    if count <= 4:
        for i in range(count):
            body(i)
    else:
        def step(i, carry):
            body(i)
            return carry
        lax.fori_loop(0, count, step, 0)


def kernel(
    n, particles, defocus, noise_hbm, references, starts_hbm, lens_hbm,
    expon, prefix, sgath,
    gath, dgath, refs, ctf, ctf_power, power, weighted, acc, mine, noise, starts, lens,
    own_sem, piece_sem, ref_sem, up_send, down_send, side_send, recv, side_recv,
    dup_send, ddown_send, beside_send, beside_recv, pair_recv, far_send, far_recv, s_send, s_recv,
):
    wide = 2
    deep = n // wide
    per = particles.shape[0]
    feat = particles.shape[1]
    coef = feat // 2
    size = coef // PIECES
    ori = references.shape[0]
    total_ori = n * ori
    parts = n * per
    group = wide * per
    me = lax.axis_index("orient")
    row = lax.div(me, wide)
    col = lax.rem(me, wide)
    partner = row * wide + (1 - col)
    has_up = row + 1 < deep
    has_down = row > 0

    def cut(c):
        return pl.ds(c * size, size)

    short = deep == 4
    spans = [(c, c + 1) for c in ORDER] if short else SPANS
    lowest, highest = row == 0, row == deep - 1

    def span(c):
        return pl.ds(spans[c][0] * size, (spans[c][1] - spans[c][0]) * size)

    def peer(t):
        return lax.rem(me + t, n)

    def near(act):
        act(partner)

        @pl.when(has_up)
        def _():
            act(me + wide)

        @pl.when(has_down)
        def _():
            act(me - wide)

    barrier = pltpu.get_barrier_semaphore()

    def greet(target):
        pl.semaphore_signal(barrier, inc=1, device_id={"orient": target}, device_id_type=MESH)

    near(greet)
    if short:
        @pl.when(lowest)
        def _():
            for column in range(wide):
                greet((deep - 1) * wide + column)

    order = list(range(len(spans)))
    own = pltpu.make_async_copy(particles, gath.at[me], piece_sem)
    own_d = pltpu.make_async_copy(defocus, dgath.at[me], own_sem.at[0])
    own_d.start()
    own.start()
    small = [
        pltpu.make_async_copy(noise_hbm, noise, own_sem.at[1]),
        pltpu.make_async_copy(starts_hbm, starts, own_sem.at[2]),
        pltpu.make_async_copy(lens_hbm, lens, own_sem.at[3]),
    ]
    for copy in small:
        copy.start()
    own_d.wait()
    own.wait()
    for c in ORDER:
        pltpu.make_async_copy(references.at[:, cut(c)], refs.at[:, cut(c)], ref_sem.at[c % PIECES]).start()
    greeted = 1 + has_up.astype(jnp.int32) + has_down.astype(jnp.int32)
    if short:
        greeted = greeted + wide * highest.astype(jnp.int32)
    pl.semaphore_wait(barrier, greeted)

    def remote(block, send_sem, recv_sem, target):
        return pltpu.make_async_remote_copy(
            src_ref=block, dst_ref=block, send_sem=send_sem, recv_sem=recv_sem,
            device_id={"orient": target}, device_id_type=MESH)

    def block(c, source):
        return gath.at[source, :, span(c)]

    def up(c, source):
        return remote(block(c, source), up_send, recv.at[c, lax.div(source, wide)], me + wide)

    def down(c, source):
        return remote(block(c, source), down_send, recv.at[c, lax.div(source, wide) - 1], me - wide)

    def side(c, source):
        return remote(block(c, source), side_send, side_recv.at[c], partner)

    def beside(source):
        return remote(dgath.at[source], beside_send, beside_recv, partner)

    def pair(r):
        return dgath.at[pl.ds(r * wide, wide)]

    def pair_up(r):
        return remote(pair(r), dup_send, pair_recv.at[r], me + wide)

    def pair_down(r):
        return remote(pair(r), ddown_send, pair_recv.at[r - 1], me - wide)

    def s_copy(source, target):
        return pltpu.make_async_remote_copy(
            src_ref=mine, dst_ref=sgath.at[source], send_sem=s_send, recv_sem=s_recv,
            device_id={"orient": target}, device_id_type=MESH)

    others = sgath.at[pl.ds(0, n - 1)]

    def both(c, source):
        @pl.when(has_up)
        def _():
            up(c, source).start()

        @pl.when(has_down)
        def _():
            down(c, source).start()

    def far(column):
        return remote(dgath.at[me], far_send, far_recv.at[col], column)


    if short:
        @pl.when(highest)
        def _():
            for column in range(wide):
                far(column).start()

    beside(me).start()
    for c in order:
        side(c, me).start()
        both(c, me)

    def relay_pairs(t):
        if t == 0:
            beside(partner).wait_recv()

            @pl.when(has_up)
            def _():
                pair_up(row).start()

            @pl.when(has_down)
            def _():
                pair_down(row).start()

            return

        @pl.when(row >= t)
        def _():
            pair_up(row - t).wait_recv()

            @pl.when(has_up)
            def _():
                pair_up(row - t).start()

        direct = short and t == deep - 1

        @pl.when(row + t < deep)
        def _():
            if direct:
                for column in range(wide):
                    source = (deep - 1) * wide + column
                    remote(dgath.at[source], far_send, far_recv.at[column], partner).wait_recv()
            else:
                pair_down(row + t).wait_recv()

                @pl.when(has_down & (row > 1 if short and t == deep - 2 else True))
                def _():
                    pair_down(row + t).start()

    def rise(c, t):
        @pl.when(row >= t)
        def _():
            source = (row - t) * wide + col
            up(c, source).wait_recv()

            @pl.when(has_up)
            def _():
                up(c, source).start()

            side(c, source).start()

    def fall(c, t):
        @pl.when(row + t < deep)
        def _():
            source = (row + t) * wide + col
            down(c, source).wait_recv()

            @pl.when(has_down)
            def _():
                down(c, source).start()

            side(c, source).start()

    def handle(c, t):
        rise(c, t)
        fall(c, t)

    def arrived(c):
        blocks = gath.at[pl.ds(0, deep), :, span(c)]
        remote(blocks, side_send, side_recv.at[c], partner).wait_recv()

    eye8 = lax.broadcasted_iota(jnp.int32, (per, per), 0) == lax.broadcasted_iota(jnp.int32, (per, per), 1)

    def ctf_row(r):
        columns = []
        for j in range(wide):
            columns.append(jnp.sum(jnp.where(eye8, dgath[r * wide + j], 0.0), axis=1, keepdims=True))
        d = jnp.concatenate(columns, axis=0)
        rows = pl.ds(pl.multiple_of(r * group, group), group)

        def body(k):
            index = k * size + lax.broadcasted_iota(jnp.int32, (1, size), 1)
            row_pos = lax.shift_right_logical(index, 7).astype(jnp.float32)
            col_pos = ((index & 127) - 64).astype(jnp.float32)
            freq = math.pi * (row_pos * row_pos + col_pos * col_pos) / 16384.0
            value = -sin_of(d * freq + 0.07)
            ctf[rows, cut(k)] = value
            ctf_power[rows, cut(k)] = (value * value * noise[cut(k)].reshape(1, size)).astype(jnp.bfloat16)

        for k in range(PIECES):
            body(k)

    def ctf_rows(t):
        @pl.when(row >= t)
        def _():
            ctf_row(row - t)

        @pl.when(row + t < deep)
        def _():
            ctf_row(row + t)

    def power_piece(k):
        both_parts = pl.ds(0, 2 * size)
        pltpu.make_async_copy(references.at[:, both_parts], refs.at[:, both_parts], ref_sem.at[k]).wait()

        def body(i):
            rows = pl.ds(pl.multiple_of(i * ROWS, ROWS), ROWS)
            re = refs[rows, cut(k)].astype(jnp.float32)
            im = refs[rows, cut(k + PIECES)].astype(jnp.float32)
            power[rows, cut(k)] = (re * re + im * im).astype(jnp.bfloat16)

        loop(ori // ROWS, body)

    def energy():
        total = 0.0
        for k in range(PIECES):
            total = total + lax.dot_general(
                ctf_power[:, cut(k)], power[:, cut(k)], DIMS, preferred_element_type=jnp.float32)
        acc[...] = -0.5 * total

    def cross(pieces):
        total = acc[...]
        for c in pieces:
            k = c % PIECES

            def body(i):
                rows = pl.ds(pl.multiple_of(i * group, group), group)
                raw = gath[pl.ds(i * wide, wide), :, cut(c)].astype(jnp.float32).reshape(group, size)
                weighted[rows, cut(c)] = (raw * ctf[rows, cut(k)] * noise[cut(k)].reshape(1, size)).astype(jnp.bfloat16)

            loop(deep, body)
            total = total + lax.dot_general(
                weighted[:, cut(c)], refs[:, cut(c)], DIMS, preferred_element_type=jnp.float32)
        acc[...] = total

    for k in range(PIECES):
        power_piece(k)
        if k == EARLY:
            relay_pairs(0)
    for copy in small:
        copy.wait()
    if short:
        middle = has_up & has_down
        for c in order + [len(order)]:
            if c < len(order):
                rise(c, 1)
            if c > 0:
                fall(c - 1, 1)

        ctf_row(row)

        @pl.when(middle)
        def _():
            relay_pairs(1)


        @pl.when(lowest)
        def _():
            relay_pairs(1)
            ctf_row(row + 1)

        @pl.when(highest)
        def _():
            relay_pairs(1)
            ctf_row(row - 1)

        for c in order:
            handle(c, 2)
            if c == 3:
                @pl.when(row == deep - 2)
                def _():
                    relay_pairs(2)

        @pl.when(row != deep - 2)
        def _():
            relay_pairs(2)

        @pl.when(middle)
        def _():
            ctf_row(row - 1)
            ctf_row(row + 1)
            ctf_rows(2)

        @pl.when(lowest)
        def _():
            ctf_rows(2)
            relay_pairs(3)
            ctf_rows(3)

        for c in order:
            handle(c, 3)
            if c == 1:
                @pl.when(highest)
                def _():
                    ctf_rows(2)

            if c == 3:
                @pl.when(highest)
                def _():
                    relay_pairs(3)
                    ctf_rows(3)
    else:
        for t in range(1, deep):
            relay_pairs(t)
            for c in order:
                handle(c, t)
        loop(deep, ctf_row)
    energy()
    for step in STEPS if short else [(c,) for c in order]:
        for c in step:
            arrived(c)
        cross([piece for c in step for piece in range(*spans[c])])

    scores = acc[...]
    top = jnp.max(scores, axis=1, keepdims=True)
    e = jnp.exp(scores - top)
    expon[:, :ori] = e
    eye = lax.broadcasted_iota(jnp.int32, (parts, parts), 0) == lax.broadcasted_iota(jnp.int32, (parts, parts), 1)

    def to_col(x):
        return jnp.sum(jnp.where(eye, x, 0), axis=1, keepdims=True)

    def to_row(x):
        return jnp.sum(jnp.where(eye, x, 0.0), axis=0, keepdims=True)

    start = to_col(starts[...])
    length = to_col(lens[...])
    ids = me * ori + lax.broadcasted_iota(jnp.int32, (parts, ori), 1)
    rel = ids - start
    inside = jnp.where(rel < 0, rel + total_ori, rel) < length
    first = me * ori - start
    first_inside = jnp.where(first < 0, first + total_ori, first) < length
    in_range = jnp.sum(jnp.where(inside, e, 0.0), axis=1, keepdims=True)
    ahead = jnp.sum(jnp.where(rel < 0, e, 0.0), axis=1, keepdims=True)
    ahead = jnp.where(first_inside, 0.0, ahead)
    for i, value in enumerate((top, jnp.sum(e, axis=1, keepdims=True), in_range, ahead)):
        line = to_row(value)
        mine[i : i + 1, :] = line
        sgath[me, i : i + 1, :] = line
    for t in range(1, n):
        s_copy(me, peer(t)).start()

    lanes = 128
    blocks = expon.shape[1] // lanes
    if ori < expon.shape[1]:
        expon[:, ori:] = jnp.zeros((parts, expon.shape[1] - ori), jnp.float32)
    upper = (
        lax.broadcasted_iota(jnp.int32, (lanes, lanes), 0) <= lax.broadcasted_iota(jnp.int32, (lanes, lanes), 1)
    ).astype(jnp.bfloat16)
    carry = jnp.zeros((parts, 1), jnp.float32)
    for b in range(blocks):
        x = expon[:, b * lanes : (b + 1) * lanes]
        high = x.astype(jnp.bfloat16)
        rest = x - high.astype(jnp.float32)
        mid = rest.astype(jnp.bfloat16)
        low = (rest - mid.astype(jnp.float32)).astype(jnp.bfloat16)
        run = carry
        for piece in (low, mid, high):
            run = run + jnp.dot(piece, upper, preferred_element_type=jnp.float32)
        prefix[:, b * lanes : (b + 1) * lanes] = run
        carry = run[:, lanes - 1 : lanes]

    def sent(blocks, pairs, send_sem, pair_sem):
        remote(gath.at[pl.ds(0, blocks)], send_sem, side_recv.at[0], partner).wait_send()
        remote(dgath.at[pl.ds(0, pairs * wide)], pair_sem, beside_recv, partner).wait_send()

    beside(me).wait_send()
    remote(gath.at[pl.ds(0, deep)], side_send, side_recv.at[0], partner).wait_send()
    for r in range(deep - 1):
        @pl.when(row == r)
        def _():
            sent(r + 1, r + 1, up_send, dup_send)

        @pl.when(row == deep - 1 - r)
        def _():
            skipped = short and r == deep - 2
            sent(r + 1, r if skipped else r + 1, down_send, ddown_send)

    if short:
        @pl.when(highest)
        def _():
            remote(pair(deep - 1), far_send, far_recv.at[0], partner).wait_send()

    remote(others, s_send, s_recv, partner).wait_send()
    remote(others, s_send, s_recv, partner).wait_recv()


def finish(n, expon, prefix, sgath, thresholds, posterior, cumulative, evidence, kept_mass):
    parts, ori = posterior.shape
    me = lax.axis_index("orient")
    eye = lax.broadcasted_iota(jnp.int32, (parts, parts), 0) == lax.broadcasted_iota(jnp.int32, (parts, parts), 1)

    def to_col(x):
        return jnp.sum(jnp.where(eye, x, 0), axis=1, keepdims=True)

    stats = [sgath[s] for s in range(n)]
    best = stats[0][0:1]
    for s in stats[1:]:
        best = jnp.maximum(best, s[0:1])
    scale = [jnp.exp(s[0:1] - best) for s in stats]
    base = jnp.zeros_like(best)
    my_base = base
    bases = []
    for s in range(n):
        my_base = jnp.where(me == s, base, my_base)
        bases.append(base)
        base = base + scale[s] * stats[s][1:2]
    total = base
    limit = thresholds[...].astype(jnp.float32) / 1024.0 * total
    kept = jnp.zeros_like(best)
    for s in range(n):
        left = limit - bases[s] - scale[s] * stats[s][3:4]
        kept = kept + jnp.minimum(jnp.maximum(left, 0.0), scale[s] * stats[s][2:3])
    kept_mass[...] = kept / total
    evidence[...] = best + jnp.log(total)
    my_scale = to_col(jnp.exp(sgath[me, 0:1, :] - best) / total)
    my_base = to_col(my_base / total)
    posterior[...] = expon[:, :ori] * my_scale
    cumulative[...] = my_base + prefix[:, :ori] * my_scale


def on_device(n, particles, defocus, inv_noise, references, thresholds, range_start, range_len):
    per, feat = particles.shape
    coef = feat // 2
    ori = references.shape[0]
    parts = n * per
    padded = -(-ori // 128) * 128
    chunks = 2 * PIECES
    f32, bf16 = jnp.float32, jnp.bfloat16
    vmem = pl.BlockSpec(memory_space=pltpu.VMEM)
    hbm = pl.BlockSpec(memory_space=pl.ANY)
    dma = pltpu.SemaphoreType.DMA
    expon, prefix, stats = pl.pallas_call(
        functools.partial(kernel, n),
        out_shape=(
            pltpu.VMEM((parts, padded), f32),
            pltpu.VMEM((parts, padded), f32),
            pltpu.VMEM((n, 4, parts), f32),
        ),
        in_specs=[hbm] * 6,
        out_specs=[vmem] * 3,
        scratch_shapes=[
            pltpu.VMEM((n, per, feat), bf16),
            pltpu.VMEM((n, 1, per), f32),
            pltpu.VMEM((ori, feat), bf16),
            pltpu.VMEM((parts, coef), f32),
            pltpu.VMEM((parts, coef), bf16),
            pltpu.VMEM((ori, coef), bf16),
            pltpu.VMEM((parts, feat), bf16),
            pltpu.VMEM((parts, ori), f32),
            pltpu.VMEM((4, parts), f32),
            pltpu.VMEM((coef,), f32),
            pltpu.VMEM((1, parts), jnp.int32),
            pltpu.VMEM((1, parts), jnp.int32),
            dma((4,)),
            dma,
            dma((PIECES,)),
            dma, dma, dma,
            dma((chunks, n // 2 - 1)),
            dma((chunks,)),
            dma, dma, dma, dma,
            dma((n // 2 - 1,)),
            dma,
            dma((2,)),
            dma, dma,
        ],
        compiler_params=pltpu.CompilerParams(
            collective_id=0, has_side_effects=True, vmem_limit_bytes=48 * 1024 * 1024
        ),
    )(*(
        pltpu.with_memory_space_constraint(x, pltpu.HBM) for x in (
            particles, defocus.reshape(1, per), inv_noise, references,
            range_start.reshape(1, parts), range_len.reshape(1, parts))
    ))
    outs = pl.pallas_call(
        functools.partial(finish, n),
        out_shape=(
            jax.ShapeDtypeStruct((parts, ori), f32),
            jax.ShapeDtypeStruct((parts, ori), f32),
            jax.ShapeDtypeStruct((1, parts), f32),
            jax.ShapeDtypeStruct((1, parts), f32),
        ),
        in_specs=[vmem] * 4,
        out_specs=[vmem] * 4,
        compiler_params=pltpu.CompilerParams(vmem_limit_bytes=8 * 1024 * 1024),
    )(expon, prefix, stats, thresholds.reshape(1, parts))
    return outs[0], outs[1], outs[2].reshape(parts), outs[3].reshape(parts)


def solution(mesh):
    return jax.shard_map(
        functools.partial(on_device, mesh.shape["orient"]),
        mesh=mesh,
        in_specs=(
            P(("dom", "orient"), None),
            P(("dom", "orient")),
            P(),
            P(("dom", "orient"), None),
            P("dom"),
            P("dom"),
            P("dom"),
        ),
        out_specs=(P("dom", "orient"), P("dom", "orient"), P("dom"), P("dom")),
        check_vma=False,
    )
```

```python
import functools
import math

import jax
import jax.numpy as jnp
from jax import lax
from jax.experimental import pallas as pl
from jax.experimental.pallas import tpu as pltpu
from jax.sharding import PartitionSpec as P

MESH = pl.DeviceIdType.MESH
SLAB = 384
PIECES = 3
SPANS = ((0, 4), (4, 6))
BUDGET = (4, 2, 2, 1)
STEPS = ((0,), (1, 2), (3, 4), (5,))
ORDER = tuple(c for k in range(PIECES) for c in (k, k + PIECES))


def sin_of(x):
    k = jnp.floor(x * (1.0 / math.pi) + 0.5)
    r = x - k * 3.140625
    r = r - k * 9.67502593994140625e-4
    r = r - k * 1.509957990978376432e-7
    s = r * r
    p = jnp.float32(-2.3889859e-8)
    p = p * s + 2.7525562e-6
    p = p * s - 1.9840874e-4
    p = p * s + 8.3333310e-3
    p = p * s - 1.6666667e-1
    y = r + r * s * p
    half = k * 0.5
    return jnp.where(half == jnp.floor(half), y, -y)


def loop(count, body):
    if count <= 4:
        for i in range(count):
            body(i)
    else:
        def step(i, carry):
            body(i)
            return carry
        lax.fori_loop(0, count, step, 0)


def kernel(
    n, particles, defocus, noise_hbm, references, starts_hbm, lens_hbm,
    expon, prefix, sgath,
    gath, dgath, refs, turned, ctf, ctf_power, power, weighted, acc, mine, noise, starts, lens,
    own_sem, piece_sem, ref_sem, up_send, down_send, side_send, recv, side_recv,
    dup_send, ddown_send, beside_send, beside_recv, pair_recv, far_send, far_recv, s_send, s_recv,
):
    wide = 2
    deep = n // wide
    per = particles.shape[0]
    feat = particles.shape[1]
    coef = feat // 2
    size = coef // PIECES
    ori = references.shape[0]
    total_ori = n * ori
    parts = n * per
    group = wide * per
    me = lax.axis_index("orient")
    row = lax.div(me, wide)
    col = lax.rem(me, wide)
    partner = row * wide + (1 - col)
    has_up = row + 1 < deep
    has_down = row > 0

    def cut(c):
        return pl.ds(c * size, size)

    short = deep == 4
    spans = [(c, c + 1) for c in ORDER] if short else SPANS
    lowest, highest = row == 0, row == deep - 1

    def span(c):
        return pl.ds(spans[c][0] * size, (spans[c][1] - spans[c][0]) * size)

    def peer(t):
        return lax.rem(me + t, n)

    def near(act):
        act(partner)

        @pl.when(has_up)
        def _():
            act(me + wide)

        @pl.when(has_down)
        def _():
            act(me - wide)

    barrier = pltpu.get_barrier_semaphore()

    def greet(target):
        pl.semaphore_signal(barrier, inc=1, device_id={"orient": target}, device_id_type=MESH)

    near(greet)
    if short:
        @pl.when(lowest)
        def _():
            for column in range(wide):
                greet((deep - 1) * wide + column)

    order = list(range(len(spans)))
    own = pltpu.make_async_copy(particles, gath.at[me], piece_sem)
    own_d = pltpu.make_async_copy(defocus, dgath.at[me], own_sem.at[0])
    own_d.start()
    own.start()
    small = [
        pltpu.make_async_copy(noise_hbm, noise, own_sem.at[1]),
        pltpu.make_async_copy(starts_hbm, starts, own_sem.at[2]),
        pltpu.make_async_copy(lens_hbm, lens, own_sem.at[3]),
    ]
    for copy in small:
        copy.start()
    own_d.wait()
    own.wait()
    for c in ORDER:
        pltpu.make_async_copy(references.at[:, cut(c)], refs.at[:, cut(c)], ref_sem.at[c % PIECES]).start()
    greeted = 1 + has_up.astype(jnp.int32) + has_down.astype(jnp.int32)
    if short:
        greeted = greeted + wide * highest.astype(jnp.int32)
    pl.semaphore_wait(barrier, greeted)

    def remote(block, send_sem, recv_sem, target):
        return pltpu.make_async_remote_copy(
            src_ref=block, dst_ref=block, send_sem=send_sem, recv_sem=recv_sem,
            device_id={"orient": target}, device_id_type=MESH)

    def block(c, source):
        return gath.at[source, :, span(c)]

    def up(c, source):
        return remote(block(c, source), up_send, recv.at[c, lax.div(source, wide)], me + wide)

    def down(c, source):
        return remote(block(c, source), down_send, recv.at[c, lax.div(source, wide) - 1], me - wide)

    def side(c, source):
        return remote(block(c, source), side_send, side_recv.at[c], partner)

    def beside(source):
        return remote(dgath.at[source], beside_send, beside_recv, partner)

    def pair(r):
        return dgath.at[pl.ds(r * wide, wide)]

    def pair_up(r):
        return remote(pair(r), dup_send, pair_recv.at[r], me + wide)

    def pair_down(r):
        return remote(pair(r), ddown_send, pair_recv.at[r - 1], me - wide)

    def s_copy(source, target):
        return pltpu.make_async_remote_copy(
            src_ref=mine, dst_ref=sgath.at[source], send_sem=s_send, recv_sem=s_recv,
            device_id={"orient": target}, device_id_type=MESH)

    others = sgath.at[pl.ds(0, n - 1)]

    def both(c, source):
        @pl.when(has_up)
        def _():
            up(c, source).start()

        @pl.when(has_down)
        def _():
            down(c, source).start()

    def far(column):
        return remote(dgath.at[me], far_send, far_recv.at[col], column)


    if short:
        @pl.when(highest)
        def _():
            for column in range(wide):
                far(column).start()

    beside(me).start()
    for c in order:
        side(c, me).start()
        both(c, me)

    def relay_pairs(t):
        if t == 0:
            beside(partner).wait_recv()

            @pl.when(has_up)
            def _():
                pair_up(row).start()

            @pl.when(has_down)
            def _():
                pair_down(row).start()

            return

        @pl.when(row >= t)
        def _():
            pair_up(row - t).wait_recv()

            @pl.when(has_up)
            def _():
                pair_up(row - t).start()

        direct = short and t == deep - 1

        @pl.when(row + t < deep)
        def _():
            if direct:
                for column in range(wide):
                    source = (deep - 1) * wide + column
                    remote(dgath.at[source], far_send, far_recv.at[column], partner).wait_recv()
            else:
                pair_down(row + t).wait_recv()

                @pl.when(has_down & (row > 1 if short and t == deep - 2 else True))
                def _():
                    pair_down(row + t).start()

    def rise(c, t):
        @pl.when(row >= t)
        def _():
            source = (row - t) * wide + col
            up(c, source).wait_recv()

            @pl.when(has_up)
            def _():
                up(c, source).start()

            side(c, source).start()

    def fall(c, t):
        @pl.when(row + t < deep)
        def _():
            source = (row + t) * wide + col
            down(c, source).wait_recv()

            @pl.when(has_down)
            def _():
                down(c, source).start()

            side(c, source).start()

    def handle(c, t):
        rise(c, t)
        fall(c, t)

    def arrived(c):
        blocks = gath.at[pl.ds(0, deep), :, span(c)]
        remote(blocks, side_send, side_recv.at[c], partner).wait_recv()

    eye8 = lax.broadcasted_iota(jnp.int32, (per, per), 0) == lax.broadcasted_iota(jnp.int32, (per, per), 1)

    def ctf_row(r):
        columns = []
        for j in range(wide):
            columns.append(jnp.sum(jnp.where(eye8, dgath[r * wide + j], 0.0), axis=1, keepdims=True))
        d = jnp.concatenate(columns, axis=0)
        rows = pl.ds(pl.multiple_of(r * group, group), group)

        def body(k):
            index = k * size + lax.broadcasted_iota(jnp.int32, (1, size), 1)
            row_pos = lax.shift_right_logical(index, 7).astype(jnp.float32)
            col_pos = ((index & 127) - 64).astype(jnp.float32)
            freq = math.pi * (row_pos * row_pos + col_pos * col_pos) / 16384.0
            value = -sin_of(d * freq + 0.07)
            ctf[rows, cut(k)] = value
            ctf_power[rows, cut(k)] = (value * value * noise[cut(k)].reshape(1, size)).astype(jnp.bfloat16)

        for k in range(PIECES):
            body(k)

    def ctf_rows(t):
        @pl.when(row >= t)
        def _():
            ctf_row(row - t)

        @pl.when(row + t < deep)
        def _():
            ctf_row(row + t)

    def loaded(k):
        both_parts = pl.ds(0, 2 * size)
        pltpu.make_async_copy(references.at[:, both_parts], refs.at[:, both_parts], ref_sem.at[k]).wait()

    def turn_slab(start):
        slab = pl.ds(start, SLAB)
        twin = pl.ds(start + coef, SLAB)
        re = refs[:, slab].T
        im = refs[:, twin].T
        turned[slab, :] = re
        turned[twin, :] = im
        re = re.astype(jnp.float32)
        im = im.astype(jnp.float32)
        power[slab, :] = (re * re + im * im).astype(jnp.bfloat16)

    slabs = coef // SLAB
    done = [0]

    def slab_work(count):
        for i in range(done[0], min(done[0] + count, slabs)):
            for k in range(PIECES):
                if i * SLAB <= k * size < (i + 1) * SLAB or (k and i * SLAB < k * size < (i + 1) * SLAB):
                    loaded(k)
            turn_slab(i * SLAB)
        done[0] = min(done[0] + count, slabs)

    def energy():
        total = 0.0
        for k in range(PIECES):
            total = total + jnp.dot(ctf_power[:, cut(k)], power[cut(k), :], preferred_element_type=jnp.float32)
        acc[...] = -0.5 * total

    def cross(pieces):
        total = acc[...]
        for c in pieces:
            k = c % PIECES

            def body(i):
                rows = pl.ds(pl.multiple_of(i * group, group), group)
                raw = gath[pl.ds(i * wide, wide), :, cut(c)].astype(jnp.float32).reshape(group, size)
                weighted[rows, cut(c)] = (raw * ctf[rows, cut(k)] * noise[cut(k)].reshape(1, size)).astype(jnp.bfloat16)

            loop(deep, body)
            total = total + jnp.dot(weighted[:, cut(c)], turned[cut(c), :], preferred_element_type=jnp.float32)
        acc[...] = total

    if not short:
        def slab_step(i, carry):
            turn_slab(pl.multiple_of(i * SLAB, SLAB))
            return carry

        for k in range(PIECES):
            loaded(k)
        lax.fori_loop(0, slabs, slab_step, 0)
    slab_work(BUDGET[0] if short else 0)
    relay_pairs(0)
    slab_work(BUDGET[1] if short else 0)
    for copy in small:
        copy.wait()
    if short:
        middle = has_up & has_down
        for c in order + [len(order)]:
            if c < len(order):
                rise(c, 1)
            if c > 0:
                fall(c - 1, 1)

        slab_work(BUDGET[2])
        ctf_row(row)

        @pl.when(middle)
        def _():
            relay_pairs(1)


        @pl.when(lowest)
        def _():
            relay_pairs(1)
            ctf_row(row + 1)

        @pl.when(highest)
        def _():
            relay_pairs(1)
            ctf_row(row - 1)

        slab_work(BUDGET[3])
        for c in order:
            handle(c, 2)
            if c in (2, 4):
                slab_work(1)
        relay_pairs(2)

        @pl.when(middle)
        def _():
            ctf_row(row - 1)
            ctf_row(row + 1)
            ctf_rows(2)

        @pl.when(highest)
        def _():
            ctf_rows(2)

        @pl.when(lowest)
        def _():
            ctf_rows(2)
            relay_pairs(3)
            ctf_rows(3)

        for c in order:
            handle(c, 3)
        @pl.when(highest)
        def _():
            relay_pairs(3)
            ctf_rows(3)

    else:
        for t in range(1, deep):
            relay_pairs(t)
            for c in order:
                handle(c, t)
        loop(deep, ctf_row)
    if short:
        slab_work(slabs)
    energy()
    for step in STEPS if short else [(c,) for c in order]:
        for c in step:
            arrived(c)
        cross([piece for c in step for piece in range(*spans[c])])

    scores = acc[...]
    top = jnp.max(scores, axis=1, keepdims=True)
    e = jnp.exp(scores - top)
    expon[:, :ori] = e
    eye = lax.broadcasted_iota(jnp.int32, (parts, parts), 0) == lax.broadcasted_iota(jnp.int32, (parts, parts), 1)

    def to_col(x):
        return jnp.sum(jnp.where(eye, x, 0), axis=1, keepdims=True)

    def to_row(x):
        return jnp.sum(jnp.where(eye, x, 0.0), axis=0, keepdims=True)

    start = to_col(starts[...])
    length = to_col(lens[...])
    ids = me * ori + lax.broadcasted_iota(jnp.int32, (parts, ori), 1)
    rel = ids - start
    inside = jnp.where(rel < 0, rel + total_ori, rel) < length
    first = me * ori - start
    first_inside = jnp.where(first < 0, first + total_ori, first) < length
    in_range = jnp.sum(jnp.where(inside, e, 0.0), axis=1, keepdims=True)
    ahead = jnp.sum(jnp.where(rel < 0, e, 0.0), axis=1, keepdims=True)
    ahead = jnp.where(first_inside, 0.0, ahead)
    for i, value in enumerate((top, jnp.sum(e, axis=1, keepdims=True), in_range, ahead)):
        line = to_row(value)
        mine[i : i + 1, :] = line
        sgath[me, i : i + 1, :] = line
    for t in range(1, n):
        s_copy(me, peer(t)).start()

    lanes = 128
    blocks = expon.shape[1] // lanes
    if ori < expon.shape[1]:
        expon[:, ori:] = jnp.zeros((parts, expon.shape[1] - ori), jnp.float32)
    upper = (
        lax.broadcasted_iota(jnp.int32, (lanes, lanes), 0) <= lax.broadcasted_iota(jnp.int32, (lanes, lanes), 1)
    ).astype(jnp.bfloat16)
    carry = jnp.zeros((parts, 1), jnp.float32)
    for b in range(blocks):
        x = expon[:, b * lanes : (b + 1) * lanes]
        high = x.astype(jnp.bfloat16)
        rest = x - high.astype(jnp.float32)
        mid = rest.astype(jnp.bfloat16)
        low = (rest - mid.astype(jnp.float32)).astype(jnp.bfloat16)
        run = carry
        for piece in (low, mid, high):
            run = run + jnp.dot(piece, upper, preferred_element_type=jnp.float32)
        prefix[:, b * lanes : (b + 1) * lanes] = run
        carry = run[:, lanes - 1 : lanes]

    def sent(blocks, pairs, send_sem, pair_sem):
        remote(gath.at[pl.ds(0, blocks)], send_sem, side_recv.at[0], partner).wait_send()
        remote(dgath.at[pl.ds(0, pairs * wide)], pair_sem, beside_recv, partner).wait_send()

    beside(me).wait_send()
    remote(gath.at[pl.ds(0, deep)], side_send, side_recv.at[0], partner).wait_send()
    for r in range(deep - 1):
        @pl.when(row == r)
        def _():
            sent(r + 1, r + 1, up_send, dup_send)

        @pl.when(row == deep - 1 - r)
        def _():
            skipped = short and r == deep - 2
            sent(r + 1, r if skipped else r + 1, down_send, ddown_send)

    if short:
        @pl.when(highest)
        def _():
            remote(pair(deep - 1), far_send, far_recv.at[0], partner).wait_send()

    remote(others, s_send, s_recv, partner).wait_send()
    remote(others, s_send, s_recv, partner).wait_recv()


def finish(n, expon, prefix, sgath, thresholds, posterior, cumulative, evidence, kept_mass):
    parts, ori = posterior.shape
    me = lax.axis_index("orient")
    eye = lax.broadcasted_iota(jnp.int32, (parts, parts), 0) == lax.broadcasted_iota(jnp.int32, (parts, parts), 1)

    def to_col(x):
        return jnp.sum(jnp.where(eye, x, 0), axis=1, keepdims=True)

    stats = [sgath[s] for s in range(n)]
    best = stats[0][0:1]
    for s in stats[1:]:
        best = jnp.maximum(best, s[0:1])
    scale = [jnp.exp(s[0:1] - best) for s in stats]
    base = jnp.zeros_like(best)
    my_base = base
    bases = []
    for s in range(n):
        my_base = jnp.where(me == s, base, my_base)
        bases.append(base)
        base = base + scale[s] * stats[s][1:2]
    total = base
    limit = thresholds[...].astype(jnp.float32) / 1024.0 * total
    kept = jnp.zeros_like(best)
    for s in range(n):
        left = limit - bases[s] - scale[s] * stats[s][3:4]
        kept = kept + jnp.minimum(jnp.maximum(left, 0.0), scale[s] * stats[s][2:3])
    kept_mass[...] = kept / total
    evidence[...] = best + jnp.log(total)
    my_scale = to_col(jnp.exp(sgath[me, 0:1, :] - best) / total)
    my_base = to_col(my_base / total)
    posterior[...] = expon[:, :ori] * my_scale
    cumulative[...] = my_base + prefix[:, :ori] * my_scale


def on_device(n, particles, defocus, inv_noise, references, thresholds, range_start, range_len):
    per, feat = particles.shape
    coef = feat // 2
    ori = references.shape[0]
    parts = n * per
    padded = -(-ori // 128) * 128
    chunks = 2 * PIECES
    f32, bf16 = jnp.float32, jnp.bfloat16
    vmem = pl.BlockSpec(memory_space=pltpu.VMEM)
    hbm = pl.BlockSpec(memory_space=pl.ANY)
    dma = pltpu.SemaphoreType.DMA
    expon, prefix, stats = pl.pallas_call(
        functools.partial(kernel, n),
        out_shape=(
            pltpu.VMEM((parts, padded), f32),
            pltpu.VMEM((parts, padded), f32),
            pltpu.VMEM((n, 4, parts), f32),
        ),
        in_specs=[hbm] * 6,
        out_specs=[vmem] * 3,
        scratch_shapes=[
            pltpu.VMEM((n, per, feat), bf16),
            pltpu.VMEM((n, 1, per), f32),
            pltpu.VMEM((ori, feat), bf16),
            pltpu.VMEM((feat, ori), bf16),
            pltpu.VMEM((parts, coef), f32),
            pltpu.VMEM((parts, coef), bf16),
            pltpu.VMEM((coef, ori), bf16),
            pltpu.VMEM((parts, feat), bf16),
            pltpu.VMEM((parts, ori), f32),
            pltpu.VMEM((4, parts), f32),
            pltpu.VMEM((coef,), f32),
            pltpu.VMEM((1, parts), jnp.int32),
            pltpu.VMEM((1, parts), jnp.int32),
            dma((4,)),
            dma,
            dma((PIECES,)),
            dma, dma, dma,
            dma((chunks, n // 2 - 1)),
            dma((chunks,)),
            dma, dma, dma, dma,
            dma((n // 2 - 1,)),
            dma,
            dma((2,)),
            dma, dma,
        ],
        compiler_params=pltpu.CompilerParams(
            collective_id=0, has_side_effects=True, vmem_limit_bytes=56 * 1024 * 1024
        ),
    )(*(
        pltpu.with_memory_space_constraint(x, pltpu.HBM) for x in (
            particles, defocus.reshape(1, per), inv_noise, references,
            range_start.reshape(1, parts), range_len.reshape(1, parts))
    ))
    outs = pl.pallas_call(
        functools.partial(finish, n),
        out_shape=(
            jax.ShapeDtypeStruct((parts, ori), f32),
            jax.ShapeDtypeStruct((parts, ori), f32),
            jax.ShapeDtypeStruct((1, parts), f32),
            jax.ShapeDtypeStruct((1, parts), f32),
        ),
        in_specs=[vmem] * 4,
        out_specs=[vmem] * 4,
        compiler_params=pltpu.CompilerParams(vmem_limit_bytes=8 * 1024 * 1024),
    )(expon, prefix, stats, thresholds.reshape(1, parts))
    return outs[0], outs[1], outs[2].reshape(parts), outs[3].reshape(parts)


def solution(mesh):
    return jax.shard_map(
        functools.partial(on_device, mesh.shape["orient"]),
        mesh=mesh,
        in_specs=(
            P(("dom", "orient"), None),
            P(("dom", "orient")),
            P(),
            P(("dom", "orient"), None),
            P("dom"),
            P("dom"),
            P("dom"),
        ),
        out_specs=(P("dom", "orient"), P("dom", "orient"), P("dom"), P("dom")),
        check_vma=False,
    )
```

```python
import functools
import math

import jax
import jax.numpy as jnp
from jax import lax
from jax.experimental import pallas as pl
from jax.experimental.pallas import tpu as pltpu
from jax.sharding import PartitionSpec as P

MESH = pl.DeviceIdType.MESH
SLAB = 384
PIECES = 3
SPANS = ((0, 4), (4, 6))
BOUNDS = (3, 5, 7, 8, 9, 10)
STEPS = ((0, 1), (2, 3), (4, 5))
ORDER = tuple(c for k in range(PIECES) for c in (k, k + PIECES))


def sin_of(x):
    k = jnp.floor(x * (1.0 / math.pi) + 0.5)
    r = x - k * 3.140625
    r = r - k * 9.67502593994140625e-4
    r = r - k * 1.509957990978376432e-7
    s = r * r
    p = jnp.float32(-2.3889859e-8)
    p = p * s + 2.7525562e-6
    p = p * s - 1.9840874e-4
    p = p * s + 8.3333310e-3
    p = p * s - 1.6666667e-1
    y = r + r * s * p
    half = k * 0.5
    return jnp.where(half == jnp.floor(half), y, -y)


def loop(count, body):
    if count <= 4:
        for i in range(count):
            body(i)
    else:
        def step(i, carry):
            body(i)
            return carry
        lax.fori_loop(0, count, step, 0)


def kernel(
    n, particles, defocus, noise_hbm, references, starts_hbm, lens_hbm,
    expon, prefix, sgath,
    gath, dgath, refs, turned, ctf, ctf_power, power, weighted, acc, mine, noise, starts, lens,
    own_sem, piece_sem, ref_sem, up_send, down_send, side_send, recv, side_recv,
    dup_send, ddown_send, beside_send, beside_recv, pair_recv, far_send, far_recv, s_send, s_recv,
):
    wide = 2
    deep = n // wide
    per = particles.shape[0]
    feat = particles.shape[1]
    coef = feat // 2
    size = coef // PIECES
    ori = references.shape[0]
    total_ori = n * ori
    parts = n * per
    group = wide * per
    me = lax.axis_index("orient")
    row = lax.div(me, wide)
    col = lax.rem(me, wide)
    partner = row * wide + (1 - col)
    has_up = row + 1 < deep
    has_down = row > 0

    def cut(c):
        return pl.ds(c * size, size)

    short = deep == 4
    spans = [(c, c + 1) for c in ORDER] if short else SPANS
    lowest, highest = row == 0, row == deep - 1

    def span(c):
        return pl.ds(spans[c][0] * size, (spans[c][1] - spans[c][0]) * size)

    def peer(t):
        return lax.rem(me + t, n)

    def near(act):
        act(partner)

        @pl.when(has_up)
        def _():
            act(me + wide)

        @pl.when(has_down)
        def _():
            act(me - wide)

    barrier = pltpu.get_barrier_semaphore()

    def greet(target):
        pl.semaphore_signal(barrier, inc=1, device_id={"orient": target}, device_id_type=MESH)

    near(greet)
    if short:
        @pl.when(lowest)
        def _():
            for column in range(wide):
                greet((deep - 1) * wide + column)

    order = list(range(len(spans)))
    own = pltpu.make_async_copy(particles, gath.at[me], piece_sem)
    own_d = pltpu.make_async_copy(defocus, dgath.at[me], own_sem.at[0])
    own_d.start()
    own.start()
    small = [
        pltpu.make_async_copy(noise_hbm, noise, own_sem.at[1]),
        pltpu.make_async_copy(starts_hbm, starts, own_sem.at[2]),
        pltpu.make_async_copy(lens_hbm, lens, own_sem.at[3]),
    ]
    for copy in small:
        copy.start()
    own_d.wait()
    own.wait()
    for c in ORDER:
        pltpu.make_async_copy(references.at[:, cut(c)], refs.at[:, cut(c)], ref_sem.at[c % PIECES]).start()
    greeted = 1 + has_up.astype(jnp.int32) + has_down.astype(jnp.int32)
    if short:
        greeted = greeted + wide * highest.astype(jnp.int32)
    pl.semaphore_wait(barrier, greeted)

    def remote(block, send_sem, recv_sem, target):
        return pltpu.make_async_remote_copy(
            src_ref=block, dst_ref=block, send_sem=send_sem, recv_sem=recv_sem,
            device_id={"orient": target}, device_id_type=MESH)

    def block(c, source):
        return gath.at[source, :, span(c)]

    def up(c, source):
        return remote(block(c, source), up_send, recv.at[c, lax.div(source, wide)], me + wide)

    def down(c, source):
        return remote(block(c, source), down_send, recv.at[c, lax.div(source, wide) - 1], me - wide)

    def side(c, source):
        return remote(block(c, source), side_send, side_recv.at[c], partner)

    def beside(source):
        return remote(dgath.at[source], beside_send, beside_recv, partner)

    def pair(r):
        return dgath.at[pl.ds(r * wide, wide)]

    def pair_up(r):
        return remote(pair(r), dup_send, pair_recv.at[r], me + wide)

    def pair_down(r):
        return remote(pair(r), ddown_send, pair_recv.at[r - 1], me - wide)

    def s_copy(source, target):
        return pltpu.make_async_remote_copy(
            src_ref=mine, dst_ref=sgath.at[source], send_sem=s_send, recv_sem=s_recv,
            device_id={"orient": target}, device_id_type=MESH)

    others = sgath.at[pl.ds(0, n - 1)]

    def both(c, source):
        @pl.when(has_up)
        def _():
            up(c, source).start()

        @pl.when(has_down)
        def _():
            down(c, source).start()

    def far(column):
        return remote(dgath.at[me], far_send, far_recv.at[col], column)


    if short:
        @pl.when(highest)
        def _():
            for column in range(wide):
                far(column).start()

    beside(me).start()
    for c in order:
        side(c, me).start()
        both(c, me)

    def relay_pairs(t):
        if t == 0:
            beside(partner).wait_recv()

            @pl.when(has_up)
            def _():
                pair_up(row).start()

            @pl.when(has_down)
            def _():
                pair_down(row).start()

            return

        @pl.when(row >= t)
        def _():
            pair_up(row - t).wait_recv()

            @pl.when(has_up)
            def _():
                pair_up(row - t).start()

        direct = short and t == deep - 1

        @pl.when(row + t < deep)
        def _():
            if direct:
                for column in range(wide):
                    source = (deep - 1) * wide + column
                    remote(dgath.at[source], far_send, far_recv.at[column], partner).wait_recv()
            else:
                pair_down(row + t).wait_recv()

                @pl.when(has_down & (row > 1 if short and t == deep - 2 else True))
                def _():
                    pair_down(row + t).start()

    def rise(c, t):
        @pl.when(row >= t)
        def _():
            source = (row - t) * wide + col
            up(c, source).wait_recv()

            @pl.when(has_up)
            def _():
                up(c, source).start()

            side(c, source).start()

    def fall(c, t):
        @pl.when(row + t < deep)
        def _():
            source = (row + t) * wide + col
            down(c, source).wait_recv()

            @pl.when(has_down)
            def _():
                down(c, source).start()

            side(c, source).start()

    def handle(c, t):
        rise(c, t)
        fall(c, t)

    def arrived(c):
        blocks = gath.at[pl.ds(0, deep), :, span(c)]
        remote(blocks, side_send, side_recv.at[c], partner).wait_recv()

    eye8 = lax.broadcasted_iota(jnp.int32, (per, per), 0) == lax.broadcasted_iota(jnp.int32, (per, per), 1)

    def ctf_row(r):
        columns = []
        for j in range(wide):
            columns.append(jnp.sum(jnp.where(eye8, dgath[r * wide + j], 0.0), axis=1, keepdims=True))
        d = jnp.concatenate(columns, axis=0)
        rows = pl.ds(pl.multiple_of(r * group, group), group)

        def body(k):
            index = k * size + lax.broadcasted_iota(jnp.int32, (1, size), 1)
            row_pos = lax.shift_right_logical(index, 7).astype(jnp.float32)
            col_pos = ((index & 127) - 64).astype(jnp.float32)
            freq = math.pi * (row_pos * row_pos + col_pos * col_pos) / 16384.0
            value = -sin_of(d * freq + 0.07)
            inverse = noise[cut(k)].reshape(1, size)
            ctf[rows, cut(k)] = value * inverse
            ctf_power[rows, cut(k)] = (value * value * inverse).astype(jnp.bfloat16)

        for k in range(PIECES):
            body(k)

    def ctf_rows(t):
        @pl.when(row >= t)
        def _():
            ctf_row(row - t)

        @pl.when(row + t < deep)
        def _():
            ctf_row(row + t)

    def loaded(k):
        both_parts = pl.ds(0, 2 * size)
        pltpu.make_async_copy(references.at[:, both_parts], refs.at[:, both_parts], ref_sem.at[k]).wait()

    def turn_slab(start):
        slab = pl.ds(start, SLAB)
        twin = pl.ds(start + coef, SLAB)
        re = refs[:, slab].T
        im = refs[:, twin].T
        turned[slab, :] = re
        turned[twin, :] = im
        re = re.astype(jnp.float32)
        im = im.astype(jnp.float32)
        power[slab, :] = (re * re + im * im).astype(jnp.bfloat16)

    slabs = coef // SLAB
    def turn_slabs(first, last):
        for i in range(first, min(last, slabs)):
            turn_slab(i * SLAB)

    def slab_work(first, last):
        for i in range(first, min(last, slabs)):
            for k in range(PIECES):
                if i * SLAB <= k * size < (i + 1) * SLAB:
                    loaded(k)
            turn_slab(i * SLAB)

    def energy():
        total = 0.0
        for k in range(PIECES):
            total = total + jnp.dot(ctf_power[:, cut(k)], power[cut(k), :], preferred_element_type=jnp.float32)
        acc[...] = -0.5 * total

    def cross(pieces):
        total = acc[...]
        for c in pieces:
            k = c % PIECES

            def body(i):
                rows = pl.ds(pl.multiple_of(i * group, group), group)
                raw = gath[pl.ds(i * wide, wide), :, cut(c)].astype(jnp.float32).reshape(group, size)
                weighted[rows, cut(c)] = (raw * ctf[rows, cut(k)]).astype(jnp.bfloat16)

            loop(deep, body)
            total = total + jnp.dot(weighted[:, cut(c)], turned[cut(c), :], preferred_element_type=jnp.float32)
        acc[...] = total

    if not short:
        def slab_step(i, carry):
            turn_slab(pl.multiple_of(i * SLAB, SLAB))
            return carry

        for k in range(PIECES):
            loaded(k)
        lax.fori_loop(0, slabs, slab_step, 0)
    if short:
        slab_work(0, BOUNDS[0])
    relay_pairs(0)
    if short:
        slab_work(BOUNDS[0], BOUNDS[1])
    for copy in small:
        copy.wait()
    if short:
        middle = has_up & has_down
        for c in order + [len(order)]:
            if c < len(order):
                rise(c, 1)
            if c > 0:
                fall(c - 1, 1)

        @pl.when(middle)
        def _():
            relay_pairs(1)

        @pl.when(jnp.logical_not(middle))
        def _():
            turn_slabs(BOUNDS[1], BOUNDS[2])

        ctf_row(row)


        @pl.when(lowest)
        def _():
            relay_pairs(1)
            ctf_row(row + 1)

        @pl.when(highest)
        def _():
            relay_pairs(1)
            ctf_row(row - 1)

        @pl.when(jnp.logical_not(middle))
        def _():
            for k in range(PIECES):
                if BOUNDS[2] * SLAB <= k * size:
                    loaded(k)
            turn_slabs(BOUNDS[2], BOUNDS[3])

        for c in order:
            handle(c, 2)
            if c in (2, 4):
                @pl.when(jnp.logical_not(middle))
                def _():
                    turn_slabs(BOUNDS[1 + c // 2 + 1], BOUNDS[1 + c // 2 + 2])

        @pl.when(jnp.logical_not(middle))
        def _():
            turn_slabs(BOUNDS[5], slabs)

        @pl.when(row == deep - 2)
        def _():
            relay_pairs(2)

        @pl.when(middle)
        def _():
            for k in range(PIECES):
                if BOUNDS[2] * SLAB <= k * size:
                    loaded(k)
            turn_slabs(BOUNDS[1], slabs)
        @pl.when(row != deep - 2)
        def _():
            relay_pairs(2)

        @pl.when(middle)
        def _():
            ctf_row(row - 1)
            ctf_row(row + 1)
            ctf_rows(2)

        @pl.when(highest)
        def _():
            ctf_rows(2)

        @pl.when(lowest)
        def _():
            ctf_rows(2)
            relay_pairs(3)
            ctf_rows(3)

        for c in order:
            handle(c, 3)
        @pl.when(highest)
        def _():
            relay_pairs(3)
            ctf_rows(3)

    else:
        for t in range(1, deep):
            relay_pairs(t)
            for c in order:
                handle(c, t)
        loop(deep, ctf_row)
    energy()
    for step in STEPS if short else [(c,) for c in order]:
        for c in step:
            arrived(c)
        cross([piece for c in step for piece in range(*spans[c])])

    scores = acc[...]
    top = jnp.max(scores, axis=1, keepdims=True)
    e = jnp.exp(scores - top)
    expon[:, :ori] = e
    eye = lax.broadcasted_iota(jnp.int32, (parts, parts), 0) == lax.broadcasted_iota(jnp.int32, (parts, parts), 1)

    def to_col(x):
        return jnp.sum(jnp.where(eye, x, 0), axis=1, keepdims=True)

    def to_row(x):
        return jnp.sum(jnp.where(eye, x, 0.0), axis=0, keepdims=True)

    start = to_col(starts[...])
    length = to_col(lens[...])
    ids = me * ori + lax.broadcasted_iota(jnp.int32, (parts, ori), 1)
    rel = ids - start
    inside = jnp.where(rel < 0, rel + total_ori, rel) < length
    first = me * ori - start
    first_inside = jnp.where(first < 0, first + total_ori, first) < length
    in_range = jnp.sum(jnp.where(inside, e, 0.0), axis=1, keepdims=True)
    ahead = jnp.sum(jnp.where(rel < 0, e, 0.0), axis=1, keepdims=True)
    ahead = jnp.where(first_inside, 0.0, ahead)
    for i, value in enumerate((top, jnp.sum(e, axis=1, keepdims=True), in_range, ahead)):
        line = to_row(value)
        mine[i : i + 1, :] = line
        sgath[me, i : i + 1, :] = line
    for t in range(1, n):
        s_copy(me, peer(t)).start()

    lanes = 128
    blocks = expon.shape[1] // lanes
    if ori < expon.shape[1]:
        expon[:, ori:] = jnp.zeros((parts, expon.shape[1] - ori), jnp.float32)
    upper = (
        lax.broadcasted_iota(jnp.int32, (lanes, lanes), 0) <= lax.broadcasted_iota(jnp.int32, (lanes, lanes), 1)
    ).astype(jnp.bfloat16)
    carry = jnp.zeros((parts, 1), jnp.float32)
    for b in range(blocks):
        x = expon[:, b * lanes : (b + 1) * lanes]
        high = x.astype(jnp.bfloat16)
        rest = x - high.astype(jnp.float32)
        mid = rest.astype(jnp.bfloat16)
        low = (rest - mid.astype(jnp.float32)).astype(jnp.bfloat16)
        run = carry
        for piece in (low, mid, high):
            run = run + jnp.dot(piece, upper, preferred_element_type=jnp.float32)
        prefix[:, b * lanes : (b + 1) * lanes] = run
        carry = run[:, lanes - 1 : lanes]

    def sent(blocks, pairs, send_sem, pair_sem):
        remote(gath.at[pl.ds(0, blocks)], send_sem, side_recv.at[0], partner).wait_send()
        remote(dgath.at[pl.ds(0, pairs * wide)], pair_sem, beside_recv, partner).wait_send()

    beside(me).wait_send()
    remote(gath.at[pl.ds(0, deep)], side_send, side_recv.at[0], partner).wait_send()
    for r in range(deep - 1):
        @pl.when(row == r)
        def _():
            sent(r + 1, r + 1, up_send, dup_send)

        @pl.when(row == deep - 1 - r)
        def _():
            skipped = short and r == deep - 2
            sent(r + 1, r if skipped else r + 1, down_send, ddown_send)

    if short:
        @pl.when(highest)
        def _():
            remote(pair(deep - 1), far_send, far_recv.at[0], partner).wait_send()

    remote(others, s_send, s_recv, partner).wait_send()
    remote(others, s_send, s_recv, partner).wait_recv()


def finish(n, expon, prefix, sgath, thresholds, posterior, cumulative, evidence, kept_mass):
    parts, ori = posterior.shape
    me = lax.axis_index("orient")
    eye = lax.broadcasted_iota(jnp.int32, (parts, parts), 0) == lax.broadcasted_iota(jnp.int32, (parts, parts), 1)

    def to_col(x):
        return jnp.sum(jnp.where(eye, x, 0), axis=1, keepdims=True)

    stats = [sgath[s] for s in range(n)]
    best = stats[0][0:1]
    for s in stats[1:]:
        best = jnp.maximum(best, s[0:1])
    scale = [jnp.exp(s[0:1] - best) for s in stats]
    base = jnp.zeros_like(best)
    my_base = base
    bases = []
    for s in range(n):
        my_base = jnp.where(me == s, base, my_base)
        bases.append(base)
        base = base + scale[s] * stats[s][1:2]
    total = base
    limit = thresholds[...].astype(jnp.float32) / 1024.0 * total
    kept = jnp.zeros_like(best)
    for s in range(n):
        left = limit - bases[s] - scale[s] * stats[s][3:4]
        kept = kept + jnp.minimum(jnp.maximum(left, 0.0), scale[s] * stats[s][2:3])
    kept_mass[...] = kept / total
    evidence[...] = best + jnp.log(total)
    my_scale = to_col(jnp.exp(sgath[me, 0:1, :] - best) / total)
    my_base = to_col(my_base / total)
    posterior[...] = expon[:, :ori] * my_scale
    cumulative[...] = my_base + prefix[:, :ori] * my_scale


def on_device(n, particles, defocus, inv_noise, references, thresholds, range_start, range_len):
    per, feat = particles.shape
    coef = feat // 2
    ori = references.shape[0]
    parts = n * per
    padded = -(-ori // 128) * 128
    chunks = 2 * PIECES
    f32, bf16 = jnp.float32, jnp.bfloat16
    vmem = pl.BlockSpec(memory_space=pltpu.VMEM)
    hbm = pl.BlockSpec(memory_space=pl.ANY)
    dma = pltpu.SemaphoreType.DMA
    expon, prefix, stats = pl.pallas_call(
        functools.partial(kernel, n),
        out_shape=(
            pltpu.VMEM((parts, padded), f32),
            pltpu.VMEM((parts, padded), f32),
            pltpu.VMEM((n, 4, parts), f32),
        ),
        in_specs=[hbm] * 6,
        out_specs=[vmem] * 3,
        scratch_shapes=[
            pltpu.VMEM((n, per, feat), bf16),
            pltpu.VMEM((n, 1, per), f32),
            pltpu.VMEM((ori, feat), bf16),
            pltpu.VMEM((feat, ori), bf16),
            pltpu.VMEM((parts, coef), f32),
            pltpu.VMEM((parts, coef), bf16),
            pltpu.VMEM((coef, ori), bf16),
            pltpu.VMEM((parts, feat), bf16),
            pltpu.VMEM((parts, ori), f32),
            pltpu.VMEM((4, parts), f32),
            pltpu.VMEM((coef,), f32),
            pltpu.VMEM((1, parts), jnp.int32),
            pltpu.VMEM((1, parts), jnp.int32),
            dma((4,)),
            dma,
            dma((PIECES,)),
            dma, dma, dma,
            dma((chunks, n // 2 - 1)),
            dma((chunks,)),
            dma, dma, dma, dma,
            dma((n // 2 - 1,)),
            dma,
            dma((2,)),
            dma, dma,
        ],
        compiler_params=pltpu.CompilerParams(
            collective_id=0, has_side_effects=True, vmem_limit_bytes=56 * 1024 * 1024
        ),
    )(*(
        pltpu.with_memory_space_constraint(x, pltpu.HBM) for x in (
            particles, defocus.reshape(1, per), inv_noise, references,
            range_start.reshape(1, parts), range_len.reshape(1, parts))
    ))
    outs = pl.pallas_call(
        functools.partial(finish, n),
        out_shape=(
            jax.ShapeDtypeStruct((parts, ori), f32),
            jax.ShapeDtypeStruct((parts, ori), f32),
            jax.ShapeDtypeStruct((1, parts), f32),
            jax.ShapeDtypeStruct((1, parts), f32),
        ),
        in_specs=[vmem] * 4,
        out_specs=[vmem] * 4,
        compiler_params=pltpu.CompilerParams(vmem_limit_bytes=8 * 1024 * 1024),
    )(expon, prefix, stats, thresholds.reshape(1, parts))
    return outs[0], outs[1], outs[2].reshape(parts), outs[3].reshape(parts)


def solution(mesh):
    return jax.shard_map(
        functools.partial(on_device, mesh.shape["orient"]),
        mesh=mesh,
        in_specs=(
            P(("dom", "orient"), None),
            P(("dom", "orient")),
            P(),
            P(("dom", "orient"), None),
            P("dom"),
            P("dom"),
            P("dom"),
        ),
        out_specs=(P("dom", "orient"), P("dom", "orient"), P("dom"), P("dom")),
        check_vma=False,
    )
```

```python
import functools
import math

import jax
import jax.numpy as jnp
from jax import lax
from jax.experimental import pallas as pl
from jax.experimental.pallas import tpu as pltpu
from jax.sharding import PartitionSpec as P

MESH = pl.DeviceIdType.MESH
SLAB = 384
PIECES = 3
SPANS = ((0, 4), (4, 6))
BOUNDS = (3, 5, 7, 8, 9, 10)
STEPS = ((0,), (1, 2), (3, 4, 5))
ORDER = tuple(c for k in range(PIECES) for c in (k, k + PIECES))


def sin_of(x):
    k = jnp.floor(x * (1.0 / math.pi) + 0.5)
    r = x - k * 3.140625
    r = r - k * 9.67502593994140625e-4
    r = r - k * 1.509957990978376432e-7
    s = r * r
    p = jnp.float32(-2.3889859e-8)
    p = p * s + 2.7525562e-6
    p = p * s - 1.9840874e-4
    p = p * s + 8.3333310e-3
    p = p * s - 1.6666667e-1
    y = r + r * s * p
    half = k * 0.5
    return jnp.where(half == jnp.floor(half), y, -y)


def loop(count, body):
    if count <= 4:
        for i in range(count):
            body(i)
    else:
        def step(i, carry):
            body(i)
            return carry
        lax.fori_loop(0, count, step, 0)


def kernel(
    n, particles, defocus, noise_hbm, references, starts_hbm, lens_hbm,
    expon, prefix, sgath,
    gath, dgath, refs, turned, ctf, ctf_power, power, weighted, acc, mine, noise, starts, lens,
    own_sem, piece_sem, ref_sem, up_send, down_send, side_send, recv, side_recv,
    dup_send, ddown_send, beside_send, beside_recv, pair_recv, far_send, far_recv, s_send, s_recv,
):
    wide = 2
    deep = n // wide
    per = particles.shape[0]
    feat = particles.shape[1]
    coef = feat // 2
    size = coef // PIECES
    ori = references.shape[0]
    total_ori = n * ori
    parts = n * per
    group = wide * per
    me = lax.axis_index("orient")
    row = lax.div(me, wide)
    col = lax.rem(me, wide)
    partner = row * wide + (1 - col)
    has_up = row + 1 < deep
    has_down = row > 0

    def cut(c):
        return pl.ds(c * size, size)

    short = deep == 4
    spans = [(c, c + 1) for c in ORDER] if short else SPANS
    lowest, highest = row == 0, row == deep - 1

    def span(c):
        return pl.ds(spans[c][0] * size, (spans[c][1] - spans[c][0]) * size)

    def peer(t):
        return lax.rem(me + t, n)

    def near(act):
        act(partner)

        @pl.when(has_up)
        def _():
            act(me + wide)

        @pl.when(has_down)
        def _():
            act(me - wide)

    barrier = pltpu.get_barrier_semaphore()

    def greet(target):
        pl.semaphore_signal(barrier, inc=1, device_id={"orient": target}, device_id_type=MESH)

    near(greet)
    if short:
        @pl.when(lowest)
        def _():
            for column in range(wide):
                greet((deep - 1) * wide + column)

    order = list(range(len(spans)))
    own = pltpu.make_async_copy(particles, gath.at[me], piece_sem)
    own_d = pltpu.make_async_copy(defocus, dgath.at[me], own_sem.at[0])
    own_d.start()
    own.start()
    small = [
        pltpu.make_async_copy(noise_hbm, noise, own_sem.at[1]),
        pltpu.make_async_copy(starts_hbm, starts, own_sem.at[2]),
        pltpu.make_async_copy(lens_hbm, lens, own_sem.at[3]),
    ]
    for copy in small:
        copy.start()
    own_d.wait()
    own.wait()
    for c in ORDER:
        pltpu.make_async_copy(references.at[:, cut(c)], refs.at[:, cut(c)], ref_sem.at[c % PIECES]).start()
    greeted = 1 + has_up.astype(jnp.int32) + has_down.astype(jnp.int32)
    if short:
        greeted = greeted + wide * highest.astype(jnp.int32)
    pl.semaphore_wait(barrier, greeted)

    def remote(block, send_sem, recv_sem, target):
        return pltpu.make_async_remote_copy(
            src_ref=block, dst_ref=block, send_sem=send_sem, recv_sem=recv_sem,
            device_id={"orient": target}, device_id_type=MESH)

    def block(c, source):
        return gath.at[source, :, span(c)]

    def up(c, source):
        return remote(block(c, source), up_send, recv.at[c, lax.div(source, wide)], me + wide)

    def down(c, source):
        return remote(block(c, source), down_send, recv.at[c, lax.div(source, wide) - 1], me - wide)

    def side(c, source):
        return remote(block(c, source), side_send, side_recv.at[c], partner)

    def beside(source):
        return remote(dgath.at[source], beside_send, beside_recv, partner)

    def pair(r):
        return dgath.at[pl.ds(r * wide, wide)]

    def pair_up(r):
        return remote(pair(r), dup_send, pair_recv.at[r], me + wide)

    def pair_down(r):
        return remote(pair(r), ddown_send, pair_recv.at[r - 1], me - wide)

    def s_copy(source, target):
        return pltpu.make_async_remote_copy(
            src_ref=mine, dst_ref=sgath.at[source], send_sem=s_send, recv_sem=s_recv,
            device_id={"orient": target}, device_id_type=MESH)

    others = sgath.at[pl.ds(0, n - 1)]

    def both(c, source):
        @pl.when(has_up)
        def _():
            up(c, source).start()

        @pl.when(has_down)
        def _():
            down(c, source).start()

    def far(column):
        return remote(dgath.at[me], far_send, far_recv.at[col], column)


    if short:
        @pl.when(highest)
        def _():
            for column in range(wide):
                far(column).start()

    beside(me).start()
    for c in order:
        side(c, me).start()
        both(c, me)

    def relay_pairs(t):
        if t == 0:
            beside(partner).wait_recv()

            @pl.when(has_up)
            def _():
                pair_up(row).start()

            @pl.when(has_down)
            def _():
                pair_down(row).start()

            return

        @pl.when(row >= t)
        def _():
            pair_up(row - t).wait_recv()

            @pl.when(has_up)
            def _():
                pair_up(row - t).start()

        direct = short and t == deep - 1

        @pl.when(row + t < deep)
        def _():
            if direct:
                for column in range(wide):
                    source = (deep - 1) * wide + column
                    remote(dgath.at[source], far_send, far_recv.at[column], partner).wait_recv()
            else:
                pair_down(row + t).wait_recv()

                @pl.when(has_down & (row > 1 if short and t == deep - 2 else True))
                def _():
                    pair_down(row + t).start()

    def rise(c, t):
        @pl.when(row >= t)
        def _():
            source = (row - t) * wide + col
            up(c, source).wait_recv()

            @pl.when(has_up)
            def _():
                up(c, source).start()

            side(c, source).start()

    def fall(c, t):
        @pl.when(row + t < deep)
        def _():
            source = (row + t) * wide + col
            down(c, source).wait_recv()

            @pl.when(has_down)
            def _():
                down(c, source).start()

            side(c, source).start()

    def handle(c, t):
        rise(c, t)
        fall(c, t)

    def arrived(c):
        blocks = gath.at[pl.ds(0, deep), :, span(c)]
        remote(blocks, side_send, side_recv.at[c], partner).wait_recv()

    eye8 = lax.broadcasted_iota(jnp.int32, (per, per), 0) == lax.broadcasted_iota(jnp.int32, (per, per), 1)

    def ctf_row(r):
        columns = []
        for j in range(wide):
            columns.append(jnp.sum(jnp.where(eye8, dgath[r * wide + j], 0.0), axis=1, keepdims=True))
        d = jnp.concatenate(columns, axis=0)
        rows = pl.ds(pl.multiple_of(r * group, group), group)

        def body(k):
            index = k * size + lax.broadcasted_iota(jnp.int32, (1, size), 1)
            row_pos = lax.shift_right_logical(index, 7).astype(jnp.float32)
            col_pos = ((index & 127) - 64).astype(jnp.float32)
            freq = math.pi * (row_pos * row_pos + col_pos * col_pos) / 16384.0
            value = -sin_of(d * freq + 0.07)
            inverse = noise[cut(k)].reshape(1, size)
            ctf[rows, cut(k)] = value * inverse
            ctf_power[rows, cut(k)] = (value * value * inverse).astype(jnp.bfloat16)

        for k in range(PIECES):
            body(k)

    def ctf_rows(t):
        @pl.when(row >= t)
        def _():
            ctf_row(row - t)

        @pl.when(row + t < deep)
        def _():
            ctf_row(row + t)

    def loaded(k):
        both_parts = pl.ds(0, 2 * size)
        pltpu.make_async_copy(references.at[:, both_parts], refs.at[:, both_parts], ref_sem.at[k]).wait()

    def turn_slab(start):
        slab = pl.ds(start, SLAB)
        twin = pl.ds(start + coef, SLAB)
        re = refs[:, slab].T
        im = refs[:, twin].T
        turned[slab, :] = re
        turned[twin, :] = im
        re = re.astype(jnp.float32)
        im = im.astype(jnp.float32)
        power[slab, :] = (re * re + im * im).astype(jnp.bfloat16)

    slabs = coef // SLAB
    def turn_slabs(first, last):
        for i in range(first, min(last, slabs)):
            turn_slab(i * SLAB)

    def slab_work(first, last):
        for i in range(first, min(last, slabs)):
            for k in range(PIECES):
                if i * SLAB <= k * size < (i + 1) * SLAB:
                    loaded(k)
            turn_slab(i * SLAB)

    def energy():
        total = 0.0
        for k in range(PIECES):
            total = total + jnp.dot(ctf_power[:, cut(k)], power[cut(k), :], preferred_element_type=jnp.float32)
        acc[...] = -0.5 * total

    def cross(pieces):
        total = acc[...]
        for c in pieces:
            k = c % PIECES

            def body(i):
                rows = pl.ds(pl.multiple_of(i * group, group), group)
                raw = gath[pl.ds(i * wide, wide), :, cut(c)].astype(jnp.float32).reshape(group, size)
                weighted[rows, cut(c)] = (raw * ctf[rows, cut(k)]).astype(jnp.bfloat16)

            loop(deep, body)
            total = total + jnp.dot(weighted[:, cut(c)], turned[cut(c), :], preferred_element_type=jnp.float32)
        acc[...] = total

    if not short:
        def slab_step(i, carry):
            turn_slab(pl.multiple_of(i * SLAB, SLAB))
            return carry

        for k in range(PIECES):
            loaded(k)
        lax.fori_loop(0, slabs, slab_step, 0)
    if short:
        slab_work(0, BOUNDS[0])
    relay_pairs(0)
    if short:
        slab_work(BOUNDS[0], BOUNDS[1])
    for copy in small:
        copy.wait()
    if short:
        middle = has_up & has_down
        for c in order + [len(order)]:
            if c < len(order):
                rise(c, 1)
            if c > 0:
                fall(c - 1, 1)

        @pl.when(middle)
        def _():
            relay_pairs(1)

        @pl.when(jnp.logical_not(middle))
        def _():
            turn_slabs(BOUNDS[1], BOUNDS[2])

        ctf_row(row)


        @pl.when(lowest)
        def _():
            relay_pairs(1)
            ctf_row(row + 1)

        @pl.when(highest)
        def _():
            relay_pairs(1)
            ctf_row(row - 1)

        @pl.when(jnp.logical_not(middle))
        def _():
            for k in range(PIECES):
                if BOUNDS[2] * SLAB <= k * size:
                    loaded(k)
            turn_slabs(BOUNDS[2], BOUNDS[3])

        for c in order:
            handle(c, 2)
            if c in (2, 4):
                @pl.when(jnp.logical_not(middle))
                def _():
                    turn_slabs(BOUNDS[1 + c // 2 + 1], BOUNDS[1 + c // 2 + 2])

        @pl.when(jnp.logical_not(middle))
        def _():
            turn_slabs(BOUNDS[5], slabs)

        @pl.when(row == deep - 2)
        def _():
            relay_pairs(2)

        @pl.when(middle)
        def _():
            for k in range(PIECES):
                if BOUNDS[2] * SLAB <= k * size:
                    loaded(k)
            turn_slabs(BOUNDS[1], slabs)
        @pl.when(row != deep - 2)
        def _():
            relay_pairs(2)

        @pl.when(middle)
        def _():
            ctf_row(row - 1)
            ctf_row(row + 1)
            ctf_rows(2)

        @pl.when(highest)
        def _():
            ctf_rows(2)

        @pl.when(lowest)
        def _():
            ctf_rows(2)
            relay_pairs(3)
            ctf_rows(3)

        for c in order:
            handle(c, 3)
        @pl.when(highest)
        def _():
            relay_pairs(3)
            ctf_rows(3)

    else:
        for t in range(1, deep):
            relay_pairs(t)
            for c in order:
                handle(c, t)
        loop(deep, ctf_row)
    energy()
    for step in STEPS if short else [(c,) for c in order]:
        for c in step:
            arrived(c)
        cross([piece for c in step for piece in range(*spans[c])])

    scores = acc[...]
    top = jnp.max(scores, axis=1, keepdims=True)
    e = jnp.exp(scores - top)
    expon[:, :ori] = e
    eye = lax.broadcasted_iota(jnp.int32, (parts, parts), 0) == lax.broadcasted_iota(jnp.int32, (parts, parts), 1)

    def to_col(x):
        return jnp.sum(jnp.where(eye, x, 0), axis=1, keepdims=True)

    def to_row(x):
        return jnp.sum(jnp.where(eye, x, 0.0), axis=0, keepdims=True)

    start = to_col(starts[...])
    length = to_col(lens[...])
    ids = me * ori + lax.broadcasted_iota(jnp.int32, (parts, ori), 1)
    rel = ids - start
    inside = jnp.where(rel < 0, rel + total_ori, rel) < length
    first = me * ori - start
    first_inside = jnp.where(first < 0, first + total_ori, first) < length
    in_range = jnp.sum(jnp.where(inside, e, 0.0), axis=1, keepdims=True)
    ahead = jnp.sum(jnp.where(rel < 0, e, 0.0), axis=1, keepdims=True)
    ahead = jnp.where(first_inside, 0.0, ahead)
    for i, value in enumerate((top, jnp.sum(e, axis=1, keepdims=True), in_range, ahead)):
        line = to_row(value)
        mine[i : i + 1, :] = line
        sgath[me, i : i + 1, :] = line
    for t in range(1, n):
        s_copy(me, peer(t)).start()

    lanes = 128
    blocks = expon.shape[1] // lanes
    if ori < expon.shape[1]:
        expon[:, ori:] = jnp.zeros((parts, expon.shape[1] - ori), jnp.float32)
    upper = (
        lax.broadcasted_iota(jnp.int32, (lanes, lanes), 0) <= lax.broadcasted_iota(jnp.int32, (lanes, lanes), 1)
    ).astype(jnp.bfloat16)
    carry = jnp.zeros((parts, 1), jnp.float32)
    for b in range(blocks):
        x = expon[:, b * lanes : (b + 1) * lanes]
        high = x.astype(jnp.bfloat16)
        rest = x - high.astype(jnp.float32)
        mid = rest.astype(jnp.bfloat16)
        low = (rest - mid.astype(jnp.float32)).astype(jnp.bfloat16)
        run = carry
        for piece in (low, mid, high):
            run = run + jnp.dot(piece, upper, preferred_element_type=jnp.float32)
        prefix[:, b * lanes : (b + 1) * lanes] = run
        carry = run[:, lanes - 1 : lanes]

    def sent(blocks, pairs, send_sem, pair_sem):
        remote(gath.at[pl.ds(0, blocks)], send_sem, side_recv.at[0], partner).wait_send()
        remote(dgath.at[pl.ds(0, pairs * wide)], pair_sem, beside_recv, partner).wait_send()

    beside(me).wait_send()
    remote(gath.at[pl.ds(0, deep)], side_send, side_recv.at[0], partner).wait_send()
    for r in range(deep - 1):
        @pl.when(row == r)
        def _():
            sent(r + 1, r + 1, up_send, dup_send)

        @pl.when(row == deep - 1 - r)
        def _():
            skipped = short and r == deep - 2
            sent(r + 1, r if skipped else r + 1, down_send, ddown_send)

    if short:
        @pl.when(highest)
        def _():
            remote(pair(deep - 1), far_send, far_recv.at[0], partner).wait_send()

    remote(others, s_send, s_recv, partner).wait_send()
    remote(others, s_send, s_recv, partner).wait_recv()


def finish(n, expon, prefix, sgath, thresholds, posterior, cumulative, evidence, kept_mass):
    parts, ori = posterior.shape
    me = lax.axis_index("orient")
    eye = lax.broadcasted_iota(jnp.int32, (parts, parts), 0) == lax.broadcasted_iota(jnp.int32, (parts, parts), 1)

    def to_col(x):
        return jnp.sum(jnp.where(eye, x, 0), axis=1, keepdims=True)

    stats = [sgath[s] for s in range(n)]
    best = stats[0][0:1]
    for s in stats[1:]:
        best = jnp.maximum(best, s[0:1])
    scale = [jnp.exp(s[0:1] - best) for s in stats]
    base = jnp.zeros_like(best)
    my_base = base
    bases = []
    for s in range(n):
        my_base = jnp.where(me == s, base, my_base)
        bases.append(base)
        base = base + scale[s] * stats[s][1:2]
    total = base
    limit = thresholds[...].astype(jnp.float32) / 1024.0 * total
    kept = jnp.zeros_like(best)
    for s in range(n):
        left = limit - bases[s] - scale[s] * stats[s][3:4]
        kept = kept + jnp.minimum(jnp.maximum(left, 0.0), scale[s] * stats[s][2:3])
    kept_mass[...] = kept / total
    evidence[...] = best + jnp.log(total)
    my_scale = to_col(jnp.exp(sgath[me, 0:1, :] - best) / total)
    my_base = to_col(my_base / total)
    posterior[...] = expon[:, :ori] * my_scale
    cumulative[...] = my_base + prefix[:, :ori] * my_scale


def on_device(n, particles, defocus, inv_noise, references, thresholds, range_start, range_len):
    per, feat = particles.shape
    coef = feat // 2
    ori = references.shape[0]
    parts = n * per
    padded = -(-ori // 128) * 128
    chunks = 2 * PIECES
    f32, bf16 = jnp.float32, jnp.bfloat16
    vmem = pl.BlockSpec(memory_space=pltpu.VMEM)
    hbm = pl.BlockSpec(memory_space=pl.ANY)
    dma = pltpu.SemaphoreType.DMA
    expon, prefix, stats = pl.pallas_call(
        functools.partial(kernel, n),
        out_shape=(
            pltpu.VMEM((parts, padded), f32),
            pltpu.VMEM((parts, padded), f32),
            pltpu.VMEM((n, 4, parts), f32),
        ),
        in_specs=[hbm] * 6,
        out_specs=[vmem] * 3,
        scratch_shapes=[
            pltpu.VMEM((n, per, feat), bf16),
            pltpu.VMEM((n, 1, per), f32),
            pltpu.VMEM((ori, feat), bf16),
            pltpu.VMEM((feat, ori), bf16),
            pltpu.VMEM((parts, coef), f32),
            pltpu.VMEM((parts, coef), bf16),
            pltpu.VMEM((coef, ori), bf16),
            pltpu.VMEM((parts, feat), bf16),
            pltpu.VMEM((parts, ori), f32),
            pltpu.VMEM((4, parts), f32),
            pltpu.VMEM((coef,), f32),
            pltpu.VMEM((1, parts), jnp.int32),
            pltpu.VMEM((1, parts), jnp.int32),
            dma((4,)),
            dma,
            dma((PIECES,)),
            dma, dma, dma,
            dma((chunks, n // 2 - 1)),
            dma((chunks,)),
            dma, dma, dma, dma,
            dma((n // 2 - 1,)),
            dma,
            dma((2,)),
            dma, dma,
        ],
        compiler_params=pltpu.CompilerParams(
            collective_id=0, has_side_effects=True, vmem_limit_bytes=56 * 1024 * 1024
        ),
    )(*(
        pltpu.with_memory_space_constraint(x, pltpu.HBM) for x in (
            particles, defocus.reshape(1, per), inv_noise, references,
            range_start.reshape(1, parts), range_len.reshape(1, parts))
    ))
    outs = pl.pallas_call(
        functools.partial(finish, n),
        out_shape=(
            jax.ShapeDtypeStruct((parts, ori), f32),
            jax.ShapeDtypeStruct((parts, ori), f32),
            jax.ShapeDtypeStruct((1, parts), f32),
            jax.ShapeDtypeStruct((1, parts), f32),
        ),
        in_specs=[vmem] * 4,
        out_specs=[vmem] * 4,
        compiler_params=pltpu.CompilerParams(vmem_limit_bytes=8 * 1024 * 1024),
    )(expon, prefix, stats, thresholds.reshape(1, parts))
    return outs[0], outs[1], outs[2].reshape(parts), outs[3].reshape(parts)


def solution(mesh):
    return jax.shard_map(
        functools.partial(on_device, mesh.shape["orient"]),
        mesh=mesh,
        in_specs=(
            P(("dom", "orient"), None),
            P(("dom", "orient")),
            P(),
            P(("dom", "orient"), None),
            P("dom"),
            P("dom"),
            P("dom"),
        ),
        out_specs=(P("dom", "orient"), P("dom", "orient"), P("dom"), P("dom")),
        check_vma=False,
    )
```
